256 devices in a mesh: dp: 8 (over x, y_lo), fsdp: 32 (over z, y_hi, core).
Axes of the slice: x: 4, y: 4 (y_hi: 2, y_lo: 2; y = y_hi * 2 + y_lo), z: 8, core: 2. Of those that a mesh axis runs over, the one named last changes fastest.
Arguments:
- hidden: bfloat16 [131072, 4096], P(('dp', 'fsdp')), may hold values from -24 to 24
- queries: bfloat16 [131072, 2048], P(('dp', 'fsdp')), may hold values from -60 to 60
- cotangent: bfloat16 [131072, 2048], P(('dp', 'fsdp')), may hold values from -0.0390625 to 0.0390625
- point_start: bfloat16 [4096, 1024], P('fsdp', 'dp'), may hold values from -0.09375 to 0.09375
- point_mid: bfloat16 [4096, 1024], P('fsdp', 'dp'), may hold values from -0.09375 to 0.09375
- point_end: bfloat16 [4096, 1024], P('fsdp', 'dp'), may hold values from -0.09375 to 0.09375
- curve_time: float32 [1], replicated, may hold values from 0.15 to 0.85
Outputs:
- context: bfloat16 [131072, 2048], P(('dp', 'fsdp'))
- gradient: float32 [4096, 1024], P('fsdp', 'dp')
The draws below stay inside these ranges and needn't reach their ends.
All inputs are finite; a program needn't handle non-finite values.
Results may differ from the reference program's by a relative error of at most 0.0071.
Values may be sent and summed in bfloat16 or wider, within the bound.
A program may use at most 128 MiB of HBM per device.

```python
import math
import jax
import jax.numpy as jnp
from jax import lax

D = 4096
HQ = 16
KVH = 4
HD = 128
SEQ = 512
KVW = 512
TOKENS = 131072


def draw_queries(key, part):
    first_key = jax.random.fold_in(key, 0)
    base_draw = jnp.clip(jax.random.normal(first_key, (TOKENS, HQ * HD), jnp.float32), -4.0, 4.0)
    return base_draw.astype(jnp.bfloat16)


def spiked(drawn, own_key, source, target, blocks, factor):
    owner, partner = [(jnp.arange(drawn.shape[position]) // (drawn.shape[position] // blocks)).reshape([-1 if axis == position else 1 for axis in range(drawn.ndim)]) for position in (source, target)]
    chosen = jax.random.permutation(own_key, blocks)[partner]
    strong = (owner == chosen) | (owner == (partner + blocks // 2) % blocks)
    return jnp.where(strong, factor * drawn, drawn)


def levels(stream_key, extent, cuts, least, top_value):
    gain = 1.0
    for axis_at, parts in cuts:
        steps = jax.random.uniform(jax.random.fold_in(jax.random.fold_in(stream_key, 6), axis_at), (parts,), jnp.float32, least / len(cuts), top_value / len(cuts))
        gain = gain * jnp.repeat(jnp.exp(steps), extent[axis_at] // parts).reshape((-1,) + (1,) * (len(extent) - 1 - axis_at))
    return gain


def centred(own_key, dims, scale, limit, cuts=(), held_as=jnp.bfloat16):
    entries = scale * jax.random.normal(own_key, dims, jnp.float32)
    if cuts:
        entries = entries * levels(own_key, dims, cuts, -0.22, 0.18)
    return jnp.clip(entries, -limit, limit).astype(held_as)


def heavy_noise(own_key, extent, scale, reach, cuts, heavy, held_as=jnp.bfloat16):
    values = scale * jax.random.normal(own_key, extent, jnp.float32)
    if cuts:
        values = values * levels(own_key, extent, cuts, -0.22, 0.18)
    return jnp.clip(spiked(values, jax.random.fold_in(own_key, 3), *heavy), -reach, reach).astype(held_as)


def setup_inputs(seed: int = 0) -> dict:
    splits = jax.random.split(jax.random.key(seed), 8)
    return {
        "hidden": heavy_noise(splits[0], (TOKENS, D), 1.0, 24.0, ((0, 256),), (0, 1, 256, 6.0)),
        "queries": draw_queries(jax.random.fold_in(splits[7], 71), 0),
        "cotangent": centred(splits[2], (TOKENS, HQ * HD), (TOKENS ** -0.5), 0.0390625, ((0, 256),)),
        "point_start": centred(splits[3], (D, 2 * KVW), D ** -0.5, 0.09375, ((0, 32), (1, 8))),
        "point_mid": centred(splits[4], (D, 2 * KVW), D ** -0.5, 0.09375, ((0, 32), (1, 8))),
        "point_end": centred(splits[5], (D, 2 * KVW), D ** -0.5, 0.09375, ((0, 32), (1, 8))),
        "curve_time": jnp.clip(jax.random.uniform(splits[6], (1,), jnp.float32, 0.15, 0.85), 0.15, 0.85),
    }


def rope_tables(seq_len, head_dim):
    positions = jnp.arange(seq_len, dtype=jnp.float32)[:, None]
    halves_index = jnp.arange(head_dim // 2, dtype=jnp.float32)[None, :]
    inverse = jnp.exp(-(2.0 * halves_index / head_dim) * math.log(500000.0))
    angles = positions * inverse
    cosine = jnp.concatenate([jnp.cos(angles), jnp.cos(angles)], axis=1)
    sine_t = jnp.concatenate([jnp.sin(angles), jnp.sin(angles)], axis=1)
    return (cosine, sine_t)

def rotate(values_in):
    half_size = values_in.shape[-1] // 2
    return jnp.concatenate([-values_in[..., half_size:], values_in[..., :half_size]], axis=-1)

def rotate_back(values_in):
    half_size = values_in.shape[-1] // 2
    return jnp.concatenate([values_in[..., half_size:], -values_in[..., :half_size]], axis=-1)

def attend(kv_rows, query_rows, grad_rows, kv_heads, head_dim):
    seq_len = kv_rows.shape[0]
    kv_width = kv_heads * head_dim
    group_size = query_rows.shape[1] // kv_width
    width_head = group_size * head_dim
    cosine, sine_t = rope_tables(seq_len, head_dim)
    causal = jnp.arange(seq_len)[:, None] >= jnp.arange(seq_len)[None, :]
    score_scale = 1.0 / math.sqrt(head_dim)
    contexts = []
    key_grads = []
    value_grads = []
    for kv_head in range(kv_heads):
        keys_raw = kv_rows[:, kv_head * head_dim:(kv_head + 1) * head_dim].astype(jnp.float32)
        values_head = kv_rows[:, kv_width + kv_head * head_dim:kv_width + (kv_head + 1) * head_dim].astype(jnp.float32)
        keys_head = (keys_raw * cosine + rotate(keys_raw) * sine_t).astype(jnp.bfloat16).astype(jnp.float32)
        query_head = query_rows[:, kv_head * width_head:(kv_head + 1) * width_head].reshape(seq_len, group_size, head_dim).astype(jnp.float32)
        grad_head = grad_rows[:, kv_head * width_head:(kv_head + 1) * width_head].reshape(seq_len, group_size, head_dim).astype(jnp.float32)
        scores = jnp.einsum('sgd,td->gst', query_head, keys_head) * score_scale
        scores = jnp.where(causal[None], scores, -1e+30)
        top_score = lax.optimization_barrier(jnp.max(scores, axis=-1, keepdims=True))
        weights_exp = jnp.exp(scores - top_score)
        probs = weights_exp / lax.optimization_barrier(jnp.sum(weights_exp, axis=-1, keepdims=True))
        probs_low = probs.astype(jnp.bfloat16).astype(jnp.float32)
        context_head = jnp.einsum('gst,td->sgd', probs_low, values_head).astype(jnp.bfloat16)
        contexts.append(context_head.reshape(seq_len, width_head))
        prob_grad = jnp.einsum('sgd,td->gst', grad_head, values_head)
        value_grads.append(jnp.einsum('gst,sgd->td', probs_low, grad_head))
        score_grad = probs * (prob_grad - lax.optimization_barrier(jnp.sum(prob_grad * probs, axis=-1, keepdims=True))) * score_scale
        score_low = score_grad.astype(jnp.bfloat16).astype(jnp.float32)
        rot_grad = jnp.einsum('gst,sgd->td', score_low, query_head)
        key_grads.append(rot_grad * cosine + rotate_back(rot_grad * sine_t))
    context_rows = jnp.concatenate(contexts, axis=1)
    kv_grad = jnp.concatenate(key_grads + value_grads, axis=1).astype(jnp.bfloat16)
    return (context_rows, kv_grad)

def reference(hidden, queries, cotangent, point_start, point_mid, point_end, curve_time):
    t_value = curve_time[0]
    blended = ((1.0 - t_value) ** 2 * point_start.astype(jnp.float32) + 2.0 * t_value * (1.0 - t_value) * point_mid.astype(jnp.float32) + t_value ** 2 * point_end.astype(jnp.float32)).astype(jnp.bfloat16)
    kv_rows = jnp.dot(hidden, blended, preferred_element_type=jnp.float32).astype(jnp.bfloat16)
    seq_count = hidden.shape[0] // SEQ

    def one_sequence(items):
        return attend(items[0], items[1], items[2], KVH, HD)
    context_all, grad_all = lax.map(one_sequence, (kv_rows.reshape(seq_count, SEQ, -1), queries.reshape(seq_count, SEQ, -1), cotangent.reshape(seq_count, SEQ, -1)))
    context = context_all.reshape(hidden.shape[0], -1)
    kv_grad = grad_all.reshape(hidden.shape[0], -1)
    gradient = jnp.dot(hidden.T, kv_grad, preferred_element_type=jnp.float32) * (2.0 * t_value * (1.0 - t_value))
    return (context, gradient)
```

```python
import math

import jax
import jax.numpy as jnp
import numpy as np
from jax import lax
from jax.experimental import pallas as pl
from jax.experimental.pallas import tpu as pltpu
from jax.sharding import PartitionSpec as P

KVH = 4
HD = 128
SEQ = 512
BF = jnp.bfloat16
F32 = jnp.float32
NZ = 8
STEPS = 8
DEPTH = 5
MESH = pl.DeviceIdType.MESH
NT = (((1,), (1,)), ((), ()))
TN = (((0,), (0,)), ((), ()))


def coordinates():
    dp = lax.axis_index("dp")
    fsdp = lax.axis_index("fsdp")
    x = dp // 2
    y = (fsdp // 2) % 2 * 2 + dp % 2
    z = fsdp // 4
    c = fsdp % 2
    return x, y, z, c


def device(x, y, z, c):
    return (x * 2 + y % 2, (z * 2 + y // 2) * 2 + c)


def offset(step):
    return (step + 1) // 2 * (2 * (step % 2) - 1)


class Ring:
    def __init__(self, colour, x, y, z, c):
        self.colour = colour
        self.x, self.y, self.z, self.c = x, y, z, c
        self.p1, self.p2 = (y, x) if colour == 0 else (x, y)

    def along1(self, shift):
        if self.colour == 0:
            return device(self.x, (self.y + shift + 4) % 4, self.z, self.c)
        return device((self.x + shift + 4) % 4, self.y, self.z, self.c)

    def along2(self, shift):
        if self.colour == 0:
            return device((self.x + shift + 4) % 4, self.y, self.z, self.c)
        return device(self.x, (self.y + shift + 4) % 4, self.z, self.c)


def remote(src, dst, send, recv, target):
    return pltpu.make_async_remote_copy(
        src_ref=src, dst_ref=dst, send_sem=send, recv_sem=recv, device_id=target, device_id_type=MESH
    )


def greet(x, y, z, c):
    barrier = pltpu.get_barrier_semaphore()
    peers = [device(x, y, (z + shift) % NZ, c) for shift in range(1, NZ)]
    peers += [device((x + shift) % 4, y, z, c) for shift in (1, 3)]
    peers += [device(x, (y + shift) % 4, z, c) for shift in (1, 3)]
    peers += [device(x, y, z, 1 - c)]
    for peer in peers:
        pl.semaphore_signal(barrier, inc=1, device_id=peer, device_id_type=MESH)
    return barrier, len(peers)


def project_kernel(
    start_ref, mid_ref, end_ref, time_ref, hidden_hbm, out_ref,
    hidden, buf, acc, zs, zr, as_, ar, bs, br, ds_, dr, hsem,
):
    x, y, z, c = coordinates()
    barrier, count = greet(x, y, z, c)
    load = pltpu.make_async_copy(hidden_hbm, hidden, hsem)
    load.start()
    t = time_ref[0]
    blended = (
        (1.0 - t) ** 2 * start_ref[...].astype(F32)
        + 2.0 * t * (1.0 - t) * mid_ref[...].astype(F32)
        + t**2 * end_ref[...].astype(F32)
    ).astype(BF)
    buf[0, z, c, x, y] = blended[:64]
    buf[1, z, c, y, x] = blended[64:]
    acc[...] = jnp.zeros_like(acc)
    rings = [Ring(k, x, y, z, c) for k in range(2)]
    pl.semaphore_wait(barrier, count)

    def zcopy(k, s):
        ring = rings[k]
        block = buf.at[k, z, c, ring.p2, ring.p1]
        return remote(block, block, zs.at[k, s], zr.at[k, s], device(x, y, (z - offset(s) + NZ) % NZ, c))

    def near1(k, s, way):
        ring = rings[k]
        block = buf.at[k, (z + offset(s) + NZ) % NZ, c, ring.p2, ring.p1]
        return remote(block, block, as_.at[k, s, way], ar.at[k, s, way], ring.along1(1 - 2 * way))

    def far1(k, s):
        ring = rings[k]
        shift = 1 - 2 * (s % 2)
        block = buf.at[k, (z + offset(s) + NZ) % NZ, c, ring.p2, (ring.p1 - shift + 4) % 4]
        return remote(block, block, as_.at[k, s, 2], ar.at[k, s, 2], ring.along1(shift))

    def near2(k, s, way):
        ring = rings[k]
        block = buf.at[k, (z + offset(s) + NZ) % NZ, c, ring.p2]
        return remote(block, block, bs.at[k, s, way], br.at[k, s, way], ring.along2(1 - 2 * way))

    def far2(k, s):
        ring = rings[k]
        shift = 1 - 2 * (s % 2)
        block = buf.at[k, (z + offset(s) + NZ) % NZ, c, (ring.p2 - shift + 4) % 4]
        return remote(block, block, bs.at[k, s, 2], br.at[k, s, 2], ring.along2(shift))

    def cross(k, s):
        block = buf.at[k, (z + offset(s) + NZ) % NZ, c]
        return remote(block, block, ds_.at[k, s], dr.at[k, s], device(x, y, z, 1 - c))

    for s in range(1, STEPS):
        for k in range(2):
            zcopy(k, s).start()
    load.wait()

    def body(t, carry):
        @pl.when(t < STEPS)
        def _():
            @pl.when(t > 0)
            def _():
                for k in range(2):
                    zcopy(k, t).wait_recv()

            for k in range(2):
                near1(k, t, 0).start()
                near1(k, t, 1).start()

        @pl.when((t >= 1) & (t < STEPS + 1))
        def _():
            s = t - 1
            for k in range(2):
                near1(k, s, 0).wait_recv()
                near1(k, s, 1).wait_recv()
                far1(k, s).start()

        @pl.when((t >= 2) & (t < STEPS + 2))
        def _():
            s = t - 2
            for k in range(2):
                far1(k, s).wait_recv()
                near2(k, s, 0).start()
                near2(k, s, 1).start()

        @pl.when((t >= 3) & (t < STEPS + 3))
        def _():
            s = t - 3
            for k in range(2):
                near2(k, s, 0).wait_recv()
                near2(k, s, 1).wait_recv()
                far2(k, s).start()

        @pl.when((t >= 4) & (t < STEPS + 4))
        def _():
            s = t - 4
            for k in range(2):
                far2(k, s).wait_recv()
                cross(k, s).start()

        @pl.when(t >= 5)
        def _():
            s = t - 5
            for k in range(2):
                cross(k, s).wait_recv()
            zb = (z + offset(s) + NZ) % NZ
            lhs = hidden[:, pl.ds(pl.multiple_of(zb * 512, 512), 512)]
            for n in range(4):
                groups = []
                for y_hi in range(2):
                    for core in range(2):
                        for k in range(2):
                            parts = []
                            for y_lo in range(2):
                                yy = y_hi * 2 + y_lo
                                place = (n, yy) if k == 0 else (yy, n)
                                parts.append(buf[k, zb, core, place[0], place[1]])
                            groups.append(jnp.concatenate(parts, axis=1))
                rhs = jnp.concatenate(groups, axis=0)
                acc[:, n * 256 : (n + 1) * 256] += jnp.dot(lhs, rhs, preferred_element_type=F32)

        return carry

    lax.fori_loop(0, STEPS + DEPTH, body, 0)
    out_ref[...] = acc[...].astype(BF)

    def drain(s, carry):
        for k in range(2):
            @pl.when(s > 0)
            def _():
                zcopy(k, s).wait_send()

            near1(k, s, 0).wait_send()
            near1(k, s, 1).wait_send()
            far1(k, s).wait_send()
            near2(k, s, 0).wait_send()
            near2(k, s, 1).wait_send()
            far2(k, s).wait_send()
            cross(k, s).wait_send()
        return carry

    lax.fori_loop(0, STEPS, drain, 0)


def project(start, mid, end, time, hidden):
    vmem = pl.BlockSpec(memory_space=pltpu.VMEM)
    dma = pltpu.SemaphoreType.DMA
    return pl.pallas_call(
        project_kernel,
        name="gather_project",
        out_shape=jax.ShapeDtypeStruct((SEQ, 1024), BF),
        in_specs=[vmem, vmem, vmem, pl.BlockSpec(memory_space=pltpu.SMEM), pl.BlockSpec(memory_space=pl.ANY)],
        out_specs=vmem,
        scratch_shapes=[
            pltpu.VMEM((SEQ, 4096), BF),
            pltpu.VMEM((2, NZ, 2, 4, 4, 64, 128), BF),
            pltpu.VMEM((SEQ, 1024), F32),
            dma((2, STEPS)), dma((2, STEPS)),
            dma((2, STEPS, 3)), dma((2, STEPS, 3)),
            dma((2, STEPS, 3)), dma((2, STEPS, 3)),
            dma((2, STEPS)), dma((2, STEPS)),
            dma(()),
        ],
        compiler_params=pltpu.CompilerParams(collective_id=0, has_side_effects=True, vmem_limit_bytes=60 * 2**20),
    )(start, mid, end, time, hidden)


ROWS = 256
SCALE = 1.0 / math.sqrt(HD)
FOLD = SCALE * math.log2(math.e)


def attend_kernel(
    keys_ref, values_ref, query_ref, grad_ref, cos_ref, sin_ref, cost_ref, sint_ref,
    context_ref, key_grad_ref, value_grad_ref, key_acc, value_acc,
):
    raw = keys_ref[...].astype(F32)
    keys = (raw * cos_ref[...] + pltpu.roll(raw, 64, 1) * sin_ref[...]).astype(BF)
    values = values_ref[...]
    key_acc[...] = jnp.zeros_like(key_acc)
    value_acc[...] = jnp.zeros_like(value_acc)
    for tile in range(SEQ // ROWS):
        rows = slice(tile * ROWS, (tile + 1) * ROWS)
        length = (tile + 1) * ROWS
        k_t = keys[:length]
        v_t = values[:length]
        position = lax.broadcasted_iota(jnp.int32, (ROWS, length), 0) + tile * ROWS
        causal = position >= lax.broadcasted_iota(jnp.int32, (ROWS, length), 1)
        for head in range(4):
            columns = slice(head * HD, (head + 1) * HD)
            query = query_ref[rows, columns]
            grad = grad_ref[rows, columns]
            scores = lax.dot_general(query, k_t, NT, preferred_element_type=F32)
            scores = jnp.where(causal, scores, -1e30)
            top = jnp.max(scores, axis=-1, keepdims=True)
            weights = jnp.exp2((scores - top) * FOLD)
            probs = weights * (1.0 / jnp.sum(weights, axis=-1, keepdims=True))
            low = probs.astype(BF)
            context = jnp.dot(low, v_t, preferred_element_type=F32)
            context_ref[rows, columns] = context.astype(BF)
            inner = jnp.sum(context * grad.astype(F32), axis=-1, keepdims=True)
            dprobs = lax.dot_general(grad, v_t, NT, preferred_element_type=F32)
            dscores = (probs * (dprobs - inner)).astype(BF)
            value_acc[:, :length] += lax.dot_general(grad, low, TN, preferred_element_type=F32)
            key_acc[:, :length] += lax.dot_general(query, dscores, TN, preferred_element_type=F32)
    value_grad_ref[...] = value_acc[...].astype(BF)
    first = key_acc[:64] * SCALE
    second = key_acc[64:] * SCALE
    cos = cost_ref[...]
    sin = sint_ref[...]
    key_grad_ref[:64] = (first * cos + second * sin).astype(BF)
    key_grad_ref[64:] = (second * cos - first * sin).astype(BF)


def tables():
    half = HD // 2
    inverse = np.exp(-(2.0 * np.arange(half) / HD) * math.log(500000.0))
    angles = np.arange(SEQ)[:, None] * inverse[None, :]
    cos = np.cos(angles).astype(np.float32)
    sin = np.sin(angles).astype(np.float32)
    return (
        np.concatenate([cos, cos], axis=1),
        np.concatenate([-sin, sin], axis=1),
        np.ascontiguousarray(cos.T),
        np.ascontiguousarray(sin.T),
    )


def attend(kv, queries, cotangent):
    cos, sin, cost, sint = (jnp.asarray(table) for table in tables())
    whole = lambda shape: pl.BlockSpec(shape, lambda j: (0, 0))
    return pl.pallas_call(
        attend_kernel,
        name="attend",
        grid=(KVH,),
        out_shape=(
            jax.ShapeDtypeStruct((SEQ, 2048), BF),
            jax.ShapeDtypeStruct((512, SEQ), BF),
            jax.ShapeDtypeStruct((512, SEQ), BF),
        ),
        in_specs=[
            pl.BlockSpec((SEQ, HD), lambda j: (0, j)),
            pl.BlockSpec((SEQ, HD), lambda j: (0, j + KVH)),
            pl.BlockSpec((SEQ, 512), lambda j: (0, j)),
            pl.BlockSpec((SEQ, 512), lambda j: (0, j)),
            whole((SEQ, HD)), whole((SEQ, HD)), whole((HD // 2, SEQ)), whole((HD // 2, SEQ)),
        ],
        out_specs=(
            pl.BlockSpec((SEQ, 512), lambda j: (0, j)),
            pl.BlockSpec((HD, SEQ), lambda j: (j, 0)),
            pl.BlockSpec((HD, SEQ), lambda j: (j, 0)),
        ),
        scratch_shapes=[pltpu.VMEM((HD, SEQ), F32), pltpu.VMEM((HD, SEQ), F32)],
        compiler_params=pltpu.CompilerParams(vmem_limit_bytes=40 * 2**20),
    )(kv, kv, queries, cotangent, cos, sin, cost, sint)


def reduce_kernel(
    key_ref, value_ref, hidden_hbm, out_ref,
    hidden, dsend, drecv, own, total, far2r, near2r, mid, far1r, near1r, zsend, zrecv, last,
    ds_, dr, bs, br, as_, ar, zs, zr, hsem,
):
    x, y, z, c = coordinates()
    barrier, count = greet(x, y, z, c)
    load = pltpu.make_async_copy(hidden_hbm, hidden, hsem)
    load.start()
    rings = [Ring(k, x, y, z, c) for k in range(2)]

    def target(s):
        return (z + offset(7 - s) + NZ) % NZ

    def cross(k, s):
        return remote(dsend.at[s, k], drecv.at[s, k], ds_.at[k, s], dr.at[k, s], device(x, y, z, 1 - c))

    def far2(k, s):
        ring = rings[k]
        shift = 1 - 2 * (s % 2)
        return remote(
            total.at[s, k, (ring.p2 + 2) % 4], far2r.at[s, k], bs.at[k, s, 2], br.at[k, s, 2], ring.along2(shift)
        )

    def near2(k, s, way):
        ring = rings[k]
        shift = 1 - 2 * way
        return remote(
            total.at[s, k, (ring.p2 + shift + 4) % 4], near2r.at[s, k, way],
            bs.at[k, s, way], br.at[k, s, way], ring.along2(shift),
        )

    def far1(k, s):
        ring = rings[k]
        shift = 1 - 2 * (s % 2)
        return remote(
            mid.at[s, k, (ring.p1 + 2) % 4], far1r.at[s, k], as_.at[k, s, 2], ar.at[k, s, 2], ring.along1(shift)
        )

    def near1(k, s, way):
        ring = rings[k]
        shift = 1 - 2 * way
        return remote(
            mid.at[s, k, (ring.p1 + shift + 4) % 4], near1r.at[s, k, way],
            as_.at[k, s, way], ar.at[k, s, way], ring.along1(shift),
        )

    def zcopy(k, s):
        return remote(zsend.at[s, k], zrecv.at[s, k], zs.at[k, s], zr.at[k, s], device(x, y, target(s), c))

    def product(s, core, store):
        base = target(s) * 512 + core * 128
        rhs = jnp.concatenate(
            [hidden[:, pl.ds(pl.multiple_of(base + y_hi * 256, 128), 128)] for y_hi in range(2)], axis=1
        )
        for part, ref in enumerate((key_ref, value_ref)):
            grads = jnp.dot(ref[...], rhs, preferred_element_type=F32)
            for row in range(4):
                xx = part * 2 + row // 2
                for y_hi in range(2):
                    yy = y_hi * 2 + row % 2
                    lanes = slice(y_hi * 128, (y_hi + 1) * 128)
                    store(0, xx, yy, grads[row * 128 : row * 128 + 64, lanes])
                    store(1, yy, xx, grads[row * 128 + 64 : row * 128 + 128, lanes])

    pl.semaphore_wait(barrier, count)
    load.wait()

    def body(t, carry):
        @pl.when(t >= 5)
        def _():
            s = t - 5
            for k in range(2):
                near1(k, s, 0).wait_recv()
                near1(k, s, 1).wait_recv()
                summed = (
                    mid[s, k, rings[k].p1].astype(F32) + near1r[s, k, 0].astype(F32) + near1r[s, k, 1].astype(F32)
                )
                last[k] = summed
                zsend[s, k] = summed.astype(BF)

                @pl.when(s < STEPS - 1)
                def _():
                    zcopy(k, s).start()

        @pl.when((t >= 4) & (t < STEPS + 4))
        def _():
            s = t - 4
            for k in range(2):
                far1(k, s).wait_recv()
                place = (rings[k].p1 + 1 - 2 * (s % 2) + 4) % 4
                mid[s, k, place] = (mid[s, k, place].astype(F32) + far1r[s, k].astype(F32)).astype(BF)
                near1(k, s, 0).start()
                near1(k, s, 1).start()

        @pl.when((t >= 3) & (t < STEPS + 3))
        def _():
            s = t - 3
            for k in range(2):
                near2(k, s, 0).wait_recv()
                near2(k, s, 1).wait_recv()
                mid[s, k] = (
                    total[s, k, rings[k].p2].astype(F32)
                    + near2r[s, k, 0].astype(F32)
                    + near2r[s, k, 1].astype(F32)
                ).astype(BF)
                far1(k, s).start()

        @pl.when((t >= 2) & (t < STEPS + 2))
        def _():
            s = t - 2
            for k in range(2):
                far2(k, s).wait_recv()
                place = (rings[k].p2 + 1 - 2 * (s % 2) + 4) % 4
                total[s, k, place] = (total[s, k, place].astype(F32) + far2r[s, k].astype(F32)).astype(BF)
                near2(k, s, 0).start()
                near2(k, s, 1).start()

        @pl.when((t >= 1) & (t < STEPS + 1))
        def _():
            s = t - 1
            for k in range(2):
                cross(k, s).wait_recv()
                for place in range(4):
                    total[s, k, place] = (own[k, place] + drecv[s, k, place].astype(F32)).astype(BF)
                far2(k, s).start()

        @pl.when(t < STEPS)
        def _():
            def away(k, i, j, block):
                dsend[t, k, i, j] = block.astype(BF)

            def keep(k, i, j, block):
                own[k, i, j] = block

            product(t, 1 - c, away)
            for k in range(2):
                cross(k, t).start()
            product(t, c, keep)

        return carry

    lax.fori_loop(0, STEPS + DEPTH, body, 0)
    sums = []
    for k in range(2):
        value = last[k]
        for s in range(STEPS - 1):
            zcopy(k, s).wait_recv()
            value = value + zrecv[s, k].astype(F32)
        sums.append(value)
    out_ref[...] = jnp.concatenate(sums, axis=0).T

    def drain(s, carry):
        for k in range(2):
            @pl.when(s < STEPS - 1)
            def _():
                zcopy(k, s).wait_send()

            near1(k, s, 0).wait_send()
            near1(k, s, 1).wait_send()
            far1(k, s).wait_send()
            near2(k, s, 0).wait_send()
            near2(k, s, 1).wait_send()
            far2(k, s).wait_send()
            cross(k, s).wait_send()
        return carry

    lax.fori_loop(0, STEPS, drain, 0)


def reduce(key_grad, value_grad, hidden):
    vmem = pl.BlockSpec(memory_space=pltpu.VMEM)
    dma = pltpu.SemaphoreType.DMA
    return pl.pallas_call(
        reduce_kernel,
        name="gradient_reduce",
        out_shape=jax.ShapeDtypeStruct((128, 128), F32),
        in_specs=[vmem, vmem, pl.BlockSpec(memory_space=pl.ANY)],
        out_specs=vmem,
        scratch_shapes=[
            pltpu.VMEM((SEQ, 4096), BF),
            pltpu.VMEM((STEPS, 2, 4, 4, 64, 128), BF),
            pltpu.VMEM((STEPS, 2, 4, 4, 64, 128), BF),
            pltpu.VMEM((2, 4, 4, 64, 128), F32),
            pltpu.VMEM((STEPS, 2, 4, 4, 64, 128), BF),
            pltpu.VMEM((STEPS, 2, 4, 64, 128), BF),
            pltpu.VMEM((STEPS, 2, 2, 4, 64, 128), BF),
            pltpu.VMEM((STEPS, 2, 4, 64, 128), BF),
            pltpu.VMEM((STEPS, 2, 64, 128), BF),
            pltpu.VMEM((STEPS, 2, 2, 64, 128), BF),
            pltpu.VMEM((STEPS, 2, 64, 128), BF),
            pltpu.VMEM((STEPS, 2, 64, 128), BF),
            pltpu.VMEM((2, 64, 128), F32),
            dma((2, STEPS)), dma((2, STEPS)),
            dma((2, STEPS, 3)), dma((2, STEPS, 3)),
            dma((2, STEPS, 3)), dma((2, STEPS, 3)),
            dma((2, STEPS)), dma((2, STEPS)),
            dma(()),
        ],
        compiler_params=pltpu.CompilerParams(collective_id=1, has_side_effects=True, vmem_limit_bytes=60 * 2**20),
    )(key_grad, value_grad, hidden)


def local(hidden, queries, cotangent, point_start, point_mid, point_end, curve_time):
    kv = project(point_start, point_mid, point_end, curve_time, hidden)
    context, key_grad, value_grad = attend(kv, queries, cotangent)
    gradient = reduce(key_grad, value_grad, hidden)
    t_value = curve_time[0]
    return (context, gradient * (2.0 * t_value * (1.0 - t_value)))


def solution(mesh):
    return jax.shard_map(
        local,
        mesh=mesh,
        in_specs=(
            P(("dp", "fsdp"), None),
            P(("dp", "fsdp"), None),
            P(("dp", "fsdp"), None),
            P("fsdp", "dp"),
            P("fsdp", "dp"),
            P("fsdp", "dp"),
            P(),
        ),
        out_specs=(P(("dp", "fsdp"), None), P("fsdp", "dp")),
        check_vma=False,
    )
```

```python
import math

import jax
import jax.numpy as jnp
import numpy as np
from jax import lax
from jax.experimental import pallas as pl
from jax.experimental.pallas import tpu as pltpu
from jax.sharding import PartitionSpec as P

KVH = 4
HD = 128
SEQ = 512
BF = jnp.bfloat16
F32 = jnp.float32
NZ = 8
STEPS = 8
GATHER = (0, 2, 4, 6, 7)
REDUCE = (0, 1, 3, 6, 9)
MESH = pl.DeviceIdType.MESH
NT = (((1,), (1,)), ((), ()))
TN = (((0,), (0,)), ((), ()))


def coordinates():
    dp = lax.axis_index("dp")
    fsdp = lax.axis_index("fsdp")
    x = dp // 2
    y = (fsdp // 2) % 2 * 2 + dp % 2
    z = fsdp // 4
    c = fsdp % 2
    return x, y, z, c


def device(x, y, z, c):
    return (x * 2 + y % 2, (z * 2 + y // 2) * 2 + c)


def offset(step):
    return (step + 1) // 2 * (2 * (step % 2) - 1)


class Ring:
    def __init__(self, colour, x, y, z, c):
        self.colour = colour
        self.x, self.y, self.z, self.c = x, y, z, c
        self.p1, self.p2 = (y, x) if colour == 0 else (x, y)

    def along1(self, shift):
        if self.colour == 0:
            return device(self.x, (self.y + shift + 4) % 4, self.z, self.c)
        return device((self.x + shift + 4) % 4, self.y, self.z, self.c)

    def along2(self, shift):
        if self.colour == 0:
            return device((self.x + shift + 4) % 4, self.y, self.z, self.c)
        return device(self.x, (self.y + shift + 4) % 4, self.z, self.c)


def remote(src, dst, send, recv, target):
    return pltpu.make_async_remote_copy(
        src_ref=src, dst_ref=dst, send_sem=send, recv_sem=recv, device_id=target, device_id_type=MESH
    )


def greet(x, y, z, c, shifts):
    barrier = pltpu.get_barrier_semaphore()
    peers = [device(x, y, (z + shift) % NZ, c) for shift in shifts]
    peers += [device((x + shift) % 4, y, z, c) for shift in (1, 2, 3)]
    peers += [device(x, (y + shift) % 4, z, c) for shift in (1, 2, 3)]
    peers += [device(x, y, z, 1 - c)]
    for peer in peers:
        pl.semaphore_signal(barrier, inc=1, device_id=peer, device_id_type=MESH)
    return barrier, len(peers)


def pipeline(stages, starts, order):
    def body(t, carry):
        for i in order:
            @pl.when((t >= starts[i]) & (t < STEPS + starts[i]))
            def _():
                stages[i](t - starts[i])

        return carry

    lax.fori_loop(0, STEPS + starts[-1], body, 0)


def project_kernel(
    start_ref, mid_ref, end_ref, time_ref, hidden_hbm, out_ref,
    hidden, buf, acc, zs, zr, as_, ar, bs, br, ds_, dr, hsem,
):
    x, y, z, c = coordinates()
    barrier, count = greet(x, y, z, c, (1, NZ - 1))
    load = pltpu.make_async_copy(hidden_hbm, hidden, hsem)
    load.start()
    t = time_ref[0]
    blended = (
        (1.0 - t) ** 2 * start_ref[...].astype(F32)
        + 2.0 * t * (1.0 - t) * mid_ref[...].astype(F32)
        + t**2 * end_ref[...].astype(F32)
    ).astype(BF)
    buf[0, z, c, x, y] = blended[:64]
    buf[1, z, c, y, x] = blended[64:]
    acc[...] = jnp.zeros_like(acc)
    rings = [Ring(k, x, y, z, c) for k in range(2)]
    pl.semaphore_wait(barrier, count)

    def zblock(s):
        return (z + offset(s) + NZ) % NZ

    def zcopy(k, s):
        sign = 2 * (s % 2) - 1
        block = buf.at[k, (z + offset(s) - sign + NZ) % NZ, c, rings[k].p2, rings[k].p1]
        return remote(block, block, zs.at[k, s], zr.at[k, s], device(x, y, (z - sign + NZ) % NZ, c))

    def first(k, s):
        block = buf.at[k, zblock(s), c, rings[k].p2, rings[k].p1]
        return [
            remote(block, block, as_.at[k, s, i], ar.at[k, s, i], rings[k].along1(shift))
            for i, shift in enumerate((1, -1, 2))
        ]

    def near(k, s):
        block = buf.at[k, zblock(s), c, rings[k].p2]
        return [
            remote(block, block, bs.at[k, s, i], br.at[k, s, i], rings[k].along2(shift))
            for i, shift in enumerate((1, -1))
        ]

    def far(k, s):
        copies = []
        for i, shift in enumerate((1, -1)):
            block = buf.at[k, zblock(s), c, (rings[k].p2 - shift + 4) % 4, pl.ds(2 * i, 2)]
            copies.append(remote(block, block, bs.at[k, s, 2 + i], br.at[k, s, 2 + i], rings[k].along2(shift)))
        return copies

    def cross(k, s):
        block = buf.at[k, zblock(s), c]
        return remote(block, block, ds_.at[k, s], dr.at[k, s], device(x, y, z, 1 - c))

    for s in range(1, 3):
        for k in range(2):
            zcopy(k, s).start()
    load.wait()

    def stage0(s):
        @pl.when(s > 0)
        def _():
            for k in range(2):
                zcopy(k, s).wait_recv()

            @pl.when(s < STEPS - 2)
            def _():
                for k in range(2):
                    zcopy(k, s + 2).start()

        for k in range(2):
            for copy in first(k, s):
                copy.start()

    def stage1(s):
        for k in range(2):
            for copy in first(k, s):
                copy.wait_recv()
            for copy in near(k, s):
                copy.start()

    def stage2(s):
        for k in range(2):
            for copy in near(k, s):
                copy.wait_recv()
            for copy in far(k, s):
                copy.start()

    def stage3(s):
        for k in range(2):
            for copy in far(k, s):
                copy.wait_recv()
            cross(k, s).start()

    def stage4(s):
        for k in range(2):
            cross(k, s).wait_recv()
        zb = zblock(s)
        lhs = hidden[:, pl.ds(pl.multiple_of(zb * 512, 512), 512)]
        for n in range(4):
            groups = []
            for y_hi in range(2):
                for core in range(2):
                    for k in range(2):
                        parts = []
                        for y_lo in range(2):
                            yy = y_hi * 2 + y_lo
                            place = (n, yy) if k == 0 else (yy, n)
                            parts.append(buf[k, zb, core, place[0], place[1]])
                        groups.append(jnp.concatenate(parts, axis=1))
            rhs = jnp.concatenate(groups, axis=0)
            acc[:, n * 256 : (n + 1) * 256] += jnp.dot(lhs, rhs, preferred_element_type=F32)

    pipeline((stage0, stage1, stage2, stage3, stage4), GATHER, range(5))
    out_ref[...] = acc[...].astype(BF)

    def drain(s, carry):
        for k in range(2):
            @pl.when(s > 0)
            def _():
                zcopy(k, s).wait_send()

            for copy in first(k, s) + near(k, s) + far(k, s) + [cross(k, s)]:
                copy.wait_send()
        return carry

    lax.fori_loop(0, STEPS, drain, 0)


def project(start, mid, end, time, hidden):
    vmem = pl.BlockSpec(memory_space=pltpu.VMEM)
    dma = pltpu.SemaphoreType.DMA
    return pl.pallas_call(
        project_kernel,
        name="gather_project",
        out_shape=jax.ShapeDtypeStruct((SEQ, 1024), BF),
        in_specs=[vmem, vmem, vmem, pl.BlockSpec(memory_space=pltpu.SMEM), pl.BlockSpec(memory_space=pl.ANY)],
        out_specs=vmem,
        scratch_shapes=[
            pltpu.VMEM((SEQ, 4096), BF),
            pltpu.VMEM((2, NZ, 2, 4, 4, 64, 128), BF),
            pltpu.VMEM((SEQ, 1024), F32),
            dma((2, STEPS)), dma((2, STEPS)),
            dma((2, STEPS, 3)), dma((2, STEPS, 3)),
            dma((2, STEPS, 4)), dma((2, STEPS, 4)),
            dma((2, STEPS)), dma((2, STEPS)),
            dma(()),
        ],
        compiler_params=pltpu.CompilerParams(collective_id=0, has_side_effects=True, vmem_limit_bytes=60 * 2**20),
    )(start, mid, end, time, hidden)


ROWS = 256
SCALE = 1.0 / math.sqrt(HD)
FOLD = SCALE * math.log2(math.e)


def attend_kernel(
    keys_ref, values_ref, query_ref, grad_ref, cos_ref, sin_ref, cost_ref, sint_ref,
    context_ref, key_grad_ref, value_grad_ref, key_acc, value_acc,
):
    raw = keys_ref[...].astype(F32)
    keys = (raw * cos_ref[...] + pltpu.roll(raw, 64, 1) * sin_ref[...]).astype(BF)
    values = values_ref[...]
    key_acc[...] = jnp.zeros_like(key_acc)
    value_acc[...] = jnp.zeros_like(value_acc)
    causal = lax.broadcasted_iota(jnp.int32, (ROWS, ROWS), 0) >= lax.broadcasted_iota(jnp.int32, (ROWS, ROWS), 1)
    causal = jnp.concatenate([causal] * 4, axis=0)
    for tile in range(SEQ // ROWS):
        rows = slice(tile * ROWS, (tile + 1) * ROWS)
        length = (tile + 1) * ROWS
        k_t = keys[:length]
        v_t = values[:length]
        query = jnp.concatenate([query_ref[rows, h * HD : (h + 1) * HD] for h in range(4)], axis=0)
        grad = jnp.concatenate([grad_ref[rows, h * HD : (h + 1) * HD] for h in range(4)], axis=0)
        scores = lax.dot_general(query, k_t, NT, preferred_element_type=F32)
        dprobs = lax.dot_general(grad, v_t, NT, preferred_element_type=F32)
        diagonal = jnp.where(causal, scores[:, length - ROWS :], -1e30)
        scores = diagonal if tile == 0 else jnp.concatenate([scores[:, : length - ROWS], diagonal], axis=1)
        top = jnp.max(scores, axis=-1, keepdims=True)
        weights = jnp.exp2((scores - top) * FOLD)
        probs = weights * (1.0 / jnp.sum(weights, axis=-1, keepdims=True))
        low = probs.astype(BF)
        context = jnp.dot(low, v_t, preferred_element_type=F32)
        for h in range(4):
            context_ref[rows, h * HD : (h + 1) * HD] = context[h * ROWS : (h + 1) * ROWS].astype(BF)
        inner = jnp.sum(context * grad.astype(F32), axis=-1, keepdims=True)
        dscores = (probs * (dprobs - inner)).astype(BF)
        value_acc[:, :length] += lax.dot_general(grad, low, TN, preferred_element_type=F32)
        key_acc[:, :length] += lax.dot_general(query, dscores, TN, preferred_element_type=F32)
    value_grad_ref[...] = value_acc[...].astype(BF)
    first = key_acc[:64] * SCALE
    second = key_acc[64:] * SCALE
    cos = cost_ref[...]
    sin = sint_ref[...]
    key_grad_ref[:64] = (first * cos + second * sin).astype(BF)
    key_grad_ref[64:] = (second * cos - first * sin).astype(BF)


def tables():
    half = HD // 2
    inverse = np.exp(-(2.0 * np.arange(half) / HD) * math.log(500000.0))
    angles = np.arange(SEQ)[:, None] * inverse[None, :]
    cos = np.cos(angles).astype(np.float32)
    sin = np.sin(angles).astype(np.float32)
    return (
        np.concatenate([cos, cos], axis=1),
        np.concatenate([-sin, sin], axis=1),
        np.ascontiguousarray(cos.T),
        np.ascontiguousarray(sin.T),
    )


def attend(kv, queries, cotangent):
    cos, sin, cost, sint = (jnp.asarray(table) for table in tables())
    whole = lambda shape: pl.BlockSpec(shape, lambda j: (0, 0))
    return pl.pallas_call(
        attend_kernel,
        name="attend",
        grid=(KVH,),
        out_shape=(
            jax.ShapeDtypeStruct((SEQ, 2048), BF),
            jax.ShapeDtypeStruct((512, SEQ), BF),
            jax.ShapeDtypeStruct((512, SEQ), BF),
        ),
        in_specs=[
            pl.BlockSpec((SEQ, HD), lambda j: (0, j)),
            pl.BlockSpec((SEQ, HD), lambda j: (0, j + KVH)),
            pl.BlockSpec((SEQ, 512), lambda j: (0, j)),
            pl.BlockSpec((SEQ, 512), lambda j: (0, j)),
            whole((SEQ, HD)), whole((SEQ, HD)), whole((HD // 2, SEQ)), whole((HD // 2, SEQ)),
        ],
        out_specs=(
            pl.BlockSpec((SEQ, 512), lambda j: (0, j)),
            pl.BlockSpec((HD, SEQ), lambda j: (j, 0)),
            pl.BlockSpec((HD, SEQ), lambda j: (j, 0)),
        ),
        scratch_shapes=[pltpu.VMEM((HD, SEQ), F32), pltpu.VMEM((HD, SEQ), F32)],
        compiler_params=pltpu.CompilerParams(vmem_limit_bytes=60 * 2**20),
    )(kv, kv, queries, cotangent, cos, sin, cost, sint)


def reduce_kernel(
    key_ref, value_ref, hidden_hbm, out_ref,
    hidden, dsend, drecv, own, total, farr, nearr, mid, firstr, zsend, zrecv, last,
    ds_, dr, bs, br, as_, ar, zs, zr, hsem,
):
    x, y, z, c = coordinates()
    barrier, count = greet(x, y, z, c, range(1, NZ))
    load = pltpu.make_async_copy(hidden_hbm, hidden, hsem)
    load.start()
    rings = [Ring(k, x, y, z, c) for k in range(2)]

    def target(s):
        return (z + offset(7 - s) + NZ) % NZ

    def cross(k, s):
        return remote(dsend.at[s, k], drecv.at[s, k], ds_.at[k, s], dr.at[k, s], device(x, y, z, 1 - c))

    def far(k, s):
        copies = []
        for i, shift in enumerate((1, -1)):
            half = pl.ds(2 * i, 2)
            source = total.at[s, k, (rings[k].p2 + 2) % 4, half]
            copies.append(
                remote(source, farr.at[s, k, half], bs.at[k, s, 2 + i], br.at[k, s, 2 + i], rings[k].along2(shift))
            )
        return copies

    def near(k, s):
        return [
            remote(
                total.at[s, k, (rings[k].p2 + shift + 4) % 4], nearr.at[s, k, i],
                bs.at[k, s, i], br.at[k, s, i], rings[k].along2(shift),
            )
            for i, shift in enumerate((1, -1))
        ]

    def first(k, s):
        return [
            remote(
                mid.at[s, k, (rings[k].p1 + shift + 4) % 4], firstr.at[s, k, i],
                as_.at[k, s, i], ar.at[k, s, i], rings[k].along1(shift),
            )
            for i, shift in enumerate((1, -1, 2))
        ]

    def zcopy(k, s):
        return remote(zsend.at[s, k], zrecv.at[s, k], zs.at[k, s], zr.at[k, s], device(x, y, target(s), c))

    def product(s, core, store):
        base = target(s) * 512 + core * 128
        rhs = jnp.concatenate(
            [hidden[:, pl.ds(pl.multiple_of(base + y_hi * 256, 128), 128)] for y_hi in range(2)], axis=1
        )
        for part, ref in enumerate((key_ref, value_ref)):
            grads = jnp.dot(ref[...], rhs, preferred_element_type=F32)
            for row in range(4):
                xx = part * 2 + row // 2
                for y_hi in range(2):
                    yy = y_hi * 2 + row % 2
                    lanes = slice(y_hi * 128, (y_hi + 1) * 128)
                    store(0, xx, yy, grads[row * 128 : row * 128 + 64, lanes])
                    store(1, yy, xx, grads[row * 128 + 64 : row * 128 + 128, lanes])

    def give(s):
        def away(k, i, j, block):
            dsend[s, k, i, j] = block.astype(BF)

        product(s, 1 - c, away)

    def stage0(s):
        def keep(k, i, j, block):
            own[s % 4, k, i, j] = block

        @pl.when(s > 0)
        def _():
            give(s)

        for k in range(2):
            cross(k, s).start()
        product(s, c, keep)

    def stage1(s):
        for k in range(2):
            cross(k, s).wait_recv()
            for place in range(4):
                total[s, k, place] = (own[s % 4, k, place] + drecv[s, k, place].astype(F32)).astype(BF)
            for copy in far(k, s):
                copy.start()

    def stage2(s):
        for k in range(2):
            for copy in far(k, s):
                copy.wait_recv()
            for i, shift in enumerate((1, -1)):
                place = (rings[k].p2 + shift + 4) % 4
                half = slice(2 * i, 2 * i + 2)
                total[s, k, place, half] = (
                    total[s, k, place, half].astype(F32) + farr[s, k, half].astype(F32)
                ).astype(BF)
            for copy in near(k, s):
                copy.start()

    def stage3(s):
        for k in range(2):
            for copy in near(k, s):
                copy.wait_recv()
            mid[s, k] = (
                total[s, k, rings[k].p2].astype(F32) + nearr[s, k, 0].astype(F32) + nearr[s, k, 1].astype(F32)
            ).astype(BF)
            for copy in first(k, s):
                copy.start()

    def stage4(s):
        for k in range(2):
            for copy in first(k, s):
                copy.wait_recv()
            summed = mid[s, k, rings[k].p1].astype(F32)
            for i in range(3):
                summed = summed + firstr[s, k, i].astype(F32)
            last[k] = summed
            zsend[s, k] = summed.astype(BF)

        @pl.when(s < STEPS - 1)
        def _():
            for k in range(2):
                zcopy(k, s).start()

    load.wait()
    give(0)
    pl.semaphore_wait(barrier, count)
    pipeline((stage0, stage1, stage2, stage3, stage4), REDUCE, (2, 1, 3, 4, 0))
    sums = []
    for k in range(2):
        value = last[k]
        for s in range(STEPS - 1):
            zcopy(k, s).wait_recv()
            value = value + zrecv[s, k].astype(F32)
        sums.append(value)
    out_ref[...] = jnp.concatenate(sums, axis=0).T

    def drain(s, carry):
        for k in range(2):
            @pl.when(s < STEPS - 1)
            def _():
                zcopy(k, s).wait_send()

            for copy in first(k, s) + near(k, s) + far(k, s) + [cross(k, s)]:
                copy.wait_send()
        return carry

    lax.fori_loop(0, STEPS, drain, 0)


def reduce(key_grad, value_grad, hidden):
    vmem = pl.BlockSpec(memory_space=pltpu.VMEM)
    dma = pltpu.SemaphoreType.DMA
    return pl.pallas_call(
        reduce_kernel,
        name="gradient_reduce",
        out_shape=jax.ShapeDtypeStruct((128, 128), F32),
        in_specs=[vmem, vmem, pl.BlockSpec(memory_space=pl.ANY)],
        out_specs=vmem,
        scratch_shapes=[
            pltpu.VMEM((SEQ, 4096), BF),
            pltpu.VMEM((STEPS, 2, 4, 4, 64, 128), BF),
            pltpu.VMEM((STEPS, 2, 4, 4, 64, 128), BF),
            pltpu.VMEM((4, 2, 4, 4, 64, 128), F32),
            pltpu.VMEM((STEPS, 2, 4, 4, 64, 128), BF),
            pltpu.VMEM((STEPS, 2, 4, 64, 128), BF),
            pltpu.VMEM((STEPS, 2, 2, 4, 64, 128), BF),
            pltpu.VMEM((STEPS, 2, 4, 64, 128), BF),
            pltpu.VMEM((STEPS, 2, 3, 64, 128), BF),
            pltpu.VMEM((STEPS, 2, 64, 128), BF),
            pltpu.VMEM((STEPS, 2, 64, 128), BF),
            pltpu.VMEM((2, 64, 128), F32),
            dma((2, STEPS)), dma((2, STEPS)),
            dma((2, STEPS, 4)), dma((2, STEPS, 4)),
            dma((2, STEPS, 3)), dma((2, STEPS, 3)),
            dma((2, STEPS)), dma((2, STEPS)),
            dma(()),
        ],
        compiler_params=pltpu.CompilerParams(collective_id=1, has_side_effects=True, vmem_limit_bytes=60 * 2**20),
    )(key_grad, value_grad, hidden)


def local(hidden, queries, cotangent, point_start, point_mid, point_end, curve_time):
    kv = project(point_start, point_mid, point_end, curve_time, hidden)
    context, key_grad, value_grad = attend(kv, queries, cotangent)
    gradient = reduce(key_grad, value_grad, hidden)
    t_value = curve_time[0]
    return (context, gradient * (2.0 * t_value * (1.0 - t_value)))


def solution(mesh):
    return jax.shard_map(
        local,
        mesh=mesh,
        in_specs=(
            P(("dp", "fsdp"), None),
            P(("dp", "fsdp"), None),
            P(("dp", "fsdp"), None),
            P("fsdp", "dp"),
            P("fsdp", "dp"),
            P("fsdp", "dp"),
            P(),
        ),
        out_specs=(P(("dp", "fsdp"), None), P("fsdp", "dp")),
        check_vma=False,
    )
```

```python
import math

import jax
import jax.numpy as jnp
import numpy as np
from jax import lax
from jax.experimental import pallas as pl
from jax.experimental.pallas import tpu as pltpu
from jax.sharding import PartitionSpec as P

KVH = 4
HD = 128
SEQ = 512
BF = jnp.bfloat16
F32 = jnp.float32
NZ = 8
STEPS = 8
GATHER = (0, 2, 4, 6, 7)
REDUCE = (0, 1, 3, 5, 7)
PART = 56
CHAIN = 2
REST = 128 - 2 * PART
MESH = pl.DeviceIdType.MESH
NT = (((1,), (1,)), ((), ()))
TN = (((0,), (0,)), ((), ()))


def coordinates():
    dp = lax.axis_index("dp")
    fsdp = lax.axis_index("fsdp")
    x = dp // 2
    y = (fsdp // 2) % 2 * 2 + dp % 2
    z = fsdp // 4
    c = fsdp % 2
    return x, y, z, c


def device(x, y, z, c):
    return (x * 2 + y % 2, (z * 2 + y // 2) * 2 + c)


def offset(step):
    return (step + 1) // 2 * (2 * (step % 2) - 1)


class Ring:
    def __init__(self, colour, x, y, z, c):
        self.colour = colour
        self.x, self.y, self.z, self.c = x, y, z, c
        self.p1, self.p2 = (y, x) if colour == 0 else (x, y)

    def along1(self, shift):
        if self.colour == 0:
            return device(self.x, (self.y + shift + 4) % 4, self.z, self.c)
        return device((self.x + shift + 4) % 4, self.y, self.z, self.c)

    def along2(self, shift):
        if self.colour == 0:
            return device((self.x + shift + 4) % 4, self.y, self.z, self.c)
        return device(self.x, (self.y + shift + 4) % 4, self.z, self.c)


def remote(src, dst, send, recv, target):
    return pltpu.make_async_remote_copy(
        src_ref=src, dst_ref=dst, send_sem=send, recv_sem=recv, device_id=target, device_id_type=MESH
    )


def greet(x, y, z, c, shifts):
    barrier = pltpu.get_barrier_semaphore()
    peers = [device(x, y, (z + shift) % NZ, c) for shift in shifts]
    peers += [device((x + shift) % 4, y, z, c) for shift in (1, 2, 3)]
    peers += [device(x, (y + shift) % 4, z, c) for shift in (1, 2, 3)]
    peers += [device(x, y, z, 1 - c)]
    for peer in peers:
        pl.semaphore_signal(barrier, inc=1, device_id=peer, device_id_type=MESH)
    return barrier, len(peers)


def pipeline(*stages):
    def body(t, carry):
        for stage, start, first, count in stages:
            @pl.when((t >= start) & (t < start + count))
            def _():
                stage(t - start + first)

        return carry

    lax.fori_loop(0, max(start + count for _, start, _, count in stages), body, 0)


def project_kernel(
    start_ref, mid_ref, end_ref, time_ref, hidden_hbm, out_ref,
    hidden, buf, flat, acc, zs, zr, as_, ar, bs, br, ds_, dr, fs, fr, gs, gr, cs, cr, hsem,
):
    x, y, z, c = coordinates()
    barrier, count = greet(x, y, z, c, (1, NZ - 1))
    load = pltpu.make_async_copy(hidden_hbm, hidden, hsem)
    load.start()
    t = time_ref[0]
    blended = (
        (1.0 - t) ** 2 * start_ref[...].astype(F32)
        + 2.0 * t * (1.0 - t) * mid_ref[...].astype(F32)
        + t**2 * end_ref[...].astype(F32)
    ).astype(BF)
    buf[0, z, c, x, y] = blended[:PART]
    buf[1, z, c, y, x] = blended[PART : 2 * PART]
    flat[z, c, x, y] = blended[2 * PART :]
    acc[...] = jnp.zeros_like(acc)
    rings = [Ring(k, x, y, z, c) for k in range(2)]
    pl.semaphore_wait(barrier, count)

    def zblock(s):
        return (z + offset(s) + NZ) % NZ

    def zcopy(k, s):
        sign = 2 * (s % 2) - 1
        block = buf.at[k, (z + offset(s) - sign + NZ) % NZ, c, rings[k].p2, rings[k].p1]
        return remote(block, block, zs.at[k, s], zr.at[k, s], device(x, y, (z - sign + NZ) % NZ, c))

    def first(k, s):
        block = buf.at[k, zblock(s), c, rings[k].p2, rings[k].p1]
        return [
            remote(block, block, as_.at[k, s, i], ar.at[k, s, i], rings[k].along1(shift))
            for i, shift in enumerate((1, -1, 2))
        ]

    def near(k, s):
        block = buf.at[k, zblock(s), c, rings[k].p2]
        return [
            remote(block, block, bs.at[k, s, i], br.at[k, s, i], rings[k].along2(shift))
            for i, shift in enumerate((1, -1))
        ]

    def far(k, s):
        copies = []
        for i, shift in enumerate((1, -1)):
            block = buf.at[k, zblock(s), c, (rings[k].p2 - shift + 4) % 4, pl.ds(2 * i, 2)]
            copies.append(remote(block, block, bs.at[k, s, 2 + i], br.at[k, s, 2 + i], rings[k].along2(shift)))
        return copies

    def cross(k, s):
        block = buf.at[k, zblock(s), c]
        return remote(block, block, ds_.at[k, s], dr.at[k, s], device(x, y, z, 1 - c))

    def flat1():
        block = flat.at[z, c, x, y]
        return [
            remote(block, block, fs.at[i], fr.at[i], rings[0].along1(shift)) for i, shift in enumerate((1, -1, 2))
        ]

    def flat2():
        block = flat.at[z, c, x]
        return [
            remote(block, block, fs.at[3 + i], fr.at[3 + i], rings[0].along2(shift))
            for i, shift in enumerate((1, -1, 2))
        ]

    def flatz(s):
        sign = 2 * (s % 2) - 1
        block = flat.at[(z + offset(s) - sign + NZ) % NZ, c]
        return remote(block, block, gs.at[s], gr.at[s], device(x, y, (z - sign + NZ) % NZ, c))

    def flatcross(s):
        block = flat.at[zblock(s), c]
        return remote(block, block, cs.at[s], cr.at[s], device(x, y, z, 1 - c))

    for s in range(1, 3):
        for k in range(2):
            zcopy(k, s).start()
    for copy in flat1():
        copy.start()
    load.wait()

    def plane1(s):
        for copy in flat1():
            copy.wait_recv()
        for copy in flat2():
            copy.start()

    def plane2(s):
        for copy in flat2():
            copy.wait_recv()
        flatz(1).start()
        flatz(2).start()
        flatcross(0).start()

    def chain(s):
        flatz(s).wait_recv()

        @pl.when(s < STEPS - 2)
        def _():
            flatz(s + 2).start()

        flatcross(s).start()

    def stage0(s):
        @pl.when(s > 0)
        def _():
            for k in range(2):
                zcopy(k, s).wait_recv()

            @pl.when(s < STEPS - 2)
            def _():
                for k in range(2):
                    zcopy(k, s + 2).start()

        for k in range(2):
            for copy in first(k, s):
                copy.start()

    def stage1(s):
        for k in range(2):
            for copy in first(k, s):
                copy.wait_recv()
            for copy in near(k, s):
                copy.start()

    def stage2(s):
        for k in range(2):
            for copy in near(k, s):
                copy.wait_recv()
            for copy in far(k, s):
                copy.start()

    def stage3(s):
        for k in range(2):
            for copy in far(k, s):
                copy.wait_recv()
            cross(k, s).start()

    def stage4(s):
        for k in range(2):
            cross(k, s).wait_recv()
        flatcross(s).wait_recv()
        zb = zblock(s)
        lhs = hidden[:, pl.ds(pl.multiple_of(zb * 512, 512), 512)]
        for n in range(4):
            groups = []
            for y_hi in range(2):
                for core in range(2):
                    pair = (y_hi * 2, y_hi * 2 + 1)
                    groups.append(jnp.concatenate([buf[0, zb, core, n, yy] for yy in pair], axis=1))
                    groups.append(jnp.concatenate([buf[1, zb, core, yy, n] for yy in pair], axis=1))
                    groups.append(jnp.concatenate([flat[zb, core, n, yy] for yy in pair], axis=1))
            rhs = jnp.concatenate(groups, axis=0)
            acc[:, n * 256 : (n + 1) * 256] += jnp.dot(lhs, rhs, preferred_element_type=F32)

    pipeline(
        (stage0, GATHER[0], 0, STEPS),
        (stage1, GATHER[1], 0, STEPS),
        (stage2, GATHER[2], 0, STEPS),
        (stage3, GATHER[3], 0, STEPS),
        (plane1, 1, 0, 1),
        (plane2, 3, 0, 1),
        (chain, 6, 1, STEPS - 1),
        (stage4, GATHER[4], 0, STEPS),
    )
    out_ref[...] = acc[...].astype(BF)

    def drain(s, carry):
        for k in range(2):
            @pl.when(s > 0)
            def _():
                zcopy(k, s).wait_send()

            for copy in first(k, s) + near(k, s) + far(k, s) + [cross(k, s)]:
                copy.wait_send()

        @pl.when(s > 0)
        def _():
            flatz(s).wait_send()

        flatcross(s).wait_send()
        return carry

    lax.fori_loop(0, STEPS, drain, 0)
    for copy in flat1() + flat2():
        copy.wait_send()


def project(start, mid, end, time, hidden):
    vmem = pl.BlockSpec(memory_space=pltpu.VMEM)
    dma = pltpu.SemaphoreType.DMA
    return pl.pallas_call(
        project_kernel,
        name="gather_project",
        out_shape=jax.ShapeDtypeStruct((SEQ, 1024), BF),
        in_specs=[vmem, vmem, vmem, pl.BlockSpec(memory_space=pltpu.SMEM), pl.BlockSpec(memory_space=pl.ANY)],
        out_specs=vmem,
        scratch_shapes=[
            pltpu.VMEM((SEQ, 4096), BF),
            pltpu.VMEM((2, NZ, 2, 4, 4, PART, 128), BF),
            pltpu.VMEM((NZ, 2, 4, 4, REST, 128), BF),
            pltpu.VMEM((SEQ, 1024), F32),
            dma((2, STEPS)), dma((2, STEPS)),
            dma((2, STEPS, 3)), dma((2, STEPS, 3)),
            dma((2, STEPS, 4)), dma((2, STEPS, 4)),
            dma((2, STEPS)), dma((2, STEPS)),
            dma((6,)), dma((6,)),
            dma((STEPS,)), dma((STEPS,)),
            dma((STEPS,)), dma((STEPS,)),
            dma(()),
        ],
        compiler_params=pltpu.CompilerParams(collective_id=0, has_side_effects=True, vmem_limit_bytes=60 * 2**20),
    )(start, mid, end, time, hidden)


ROWS = 256
SCALE = 1.0 / math.sqrt(HD)
FOLD = SCALE * math.log2(math.e)


def attend_kernel(
    keys_ref, values_ref, query_ref, grad_ref, cos_ref, sin_ref, cost_ref, sint_ref,
    context_ref, key_grad_ref, value_grad_ref, key_acc, value_acc,
):
    raw = keys_ref[...].astype(F32)
    keys = (raw * cos_ref[...] + pltpu.roll(raw, 64, 1) * sin_ref[...]).astype(BF)
    values = values_ref[...]
    key_acc[...] = jnp.zeros_like(key_acc)
    value_acc[...] = jnp.zeros_like(value_acc)
    causal = lax.broadcasted_iota(jnp.int32, (ROWS, ROWS), 0) >= lax.broadcasted_iota(jnp.int32, (ROWS, ROWS), 1)
    causal = jnp.concatenate([causal] * 4, axis=0)
    for tile in range(SEQ // ROWS):
        rows = slice(tile * ROWS, (tile + 1) * ROWS)
        length = (tile + 1) * ROWS
        k_t = keys[:length]
        v_t = values[:length]
        query = jnp.concatenate([query_ref[rows, h * HD : (h + 1) * HD] for h in range(4)], axis=0)
        grad = jnp.concatenate([grad_ref[rows, h * HD : (h + 1) * HD] for h in range(4)], axis=0)
        scores = lax.dot_general(query, k_t, NT, preferred_element_type=F32)
        dprobs = lax.dot_general(grad, v_t, NT, preferred_element_type=F32)
        diagonal = jnp.where(causal, scores[:, length - ROWS :], -1e30)
        scores = diagonal if tile == 0 else jnp.concatenate([scores[:, : length - ROWS], diagonal], axis=1)
        top = jnp.max(scores, axis=-1, keepdims=True)
        weights = jnp.exp2((scores - top) * FOLD)
        probs = weights * (1.0 / jnp.sum(weights, axis=-1, keepdims=True))
        low = probs.astype(BF)
        context = jnp.dot(low, v_t, preferred_element_type=F32)
        for h in range(4):
            context_ref[rows, h * HD : (h + 1) * HD] = context[h * ROWS : (h + 1) * ROWS].astype(BF)
        inner = jnp.sum(context * grad.astype(F32), axis=-1, keepdims=True)
        dscores = (probs * (dprobs - inner)).astype(BF)
        value_acc[:, :length] += lax.dot_general(grad, low, TN, preferred_element_type=F32)
        key_acc[:, :length] += lax.dot_general(query, dscores, TN, preferred_element_type=F32)
    value_grad_ref[...] = value_acc[...].astype(BF)
    first = key_acc[:64] * SCALE
    second = key_acc[64:] * SCALE
    cos = cost_ref[...]
    sin = sint_ref[...]
    key_grad_ref[:64] = (first * cos + second * sin).astype(BF)
    key_grad_ref[64:] = (second * cos - first * sin).astype(BF)


def tables():
    half = HD // 2
    inverse = np.exp(-(2.0 * np.arange(half) / HD) * math.log(500000.0))
    angles = np.arange(SEQ)[:, None] * inverse[None, :]
    cos = np.cos(angles).astype(np.float32)
    sin = np.sin(angles).astype(np.float32)
    return (
        np.concatenate([cos, cos], axis=1),
        np.concatenate([-sin, sin], axis=1),
        np.ascontiguousarray(cos.T),
        np.ascontiguousarray(sin.T),
    )


def attend(kv, queries, cotangent):
    cos, sin, cost, sint = (jnp.asarray(table) for table in tables())
    whole = lambda shape: pl.BlockSpec(shape, lambda j: (0, 0))
    return pl.pallas_call(
        attend_kernel,
        name="attend",
        grid=(KVH,),
        out_shape=(
            jax.ShapeDtypeStruct((SEQ, 2048), BF),
            jax.ShapeDtypeStruct((512, SEQ), BF),
            jax.ShapeDtypeStruct((512, SEQ), BF),
        ),
        in_specs=[
            pl.BlockSpec((SEQ, HD), lambda j: (0, j)),
            pl.BlockSpec((SEQ, HD), lambda j: (0, j + KVH)),
            pl.BlockSpec((SEQ, 512), lambda j: (0, j)),
            pl.BlockSpec((SEQ, 512), lambda j: (0, j)),
            whole((SEQ, HD)), whole((SEQ, HD)), whole((HD // 2, SEQ)), whole((HD // 2, SEQ)),
        ],
        out_specs=(
            pl.BlockSpec((SEQ, 512), lambda j: (0, j)),
            pl.BlockSpec((HD, SEQ), lambda j: (j, 0)),
            pl.BlockSpec((HD, SEQ), lambda j: (j, 0)),
        ),
        scratch_shapes=[pltpu.VMEM((HD, SEQ), F32), pltpu.VMEM((HD, SEQ), F32)],
        compiler_params=pltpu.CompilerParams(vmem_limit_bytes=60 * 2**20),
    )(kv, kv, queries, cotangent, cos, sin, cost, sint)


def reduce_kernel(
    key_ref, value_ref, time_ref, hidden_hbm, out_ref,
    hidden, dsend, drecv, own, total, farr, nearr, mid, firstr, zsend, zrecv, last,
    fsend, frecv, fown, flat, flatr, slabr, line, liner,
    ds_, dr, bs, br, as_, ar, zs, zr, cs, cr, gs, gr, fs, fr, hsem,
):
    x, y, z, c = coordinates()
    barrier, count = greet(x, y, z, c, range(1, NZ))
    rings = [Ring(k, x, y, z, c) for k in range(2)]

    def target(s):
        return (z + offset(7 - s) + NZ) % NZ

    def load(s):
        columns = pl.ds(pl.multiple_of(target(s) * 512, 512), 512)
        return pltpu.make_async_copy(hidden_hbm.at[:, columns], hidden.at[:, columns], hsem.at[s])

    for s in range(STEPS):
        load(s).start()

    def cross(k, s):
        return remote(dsend.at[s, k], drecv.at[s, k], ds_.at[k, s], dr.at[k, s], device(x, y, z, 1 - c))

    def far(k, s):
        copies = []
        for i, shift in enumerate((1, -1)):
            half = pl.ds(2 * i, 2)
            source = total.at[s, k, (rings[k].p2 + 2) % 4, half]
            copies.append(
                remote(source, farr.at[s, k, half], bs.at[k, s, 2 + i], br.at[k, s, 2 + i], rings[k].along2(shift))
            )
        return copies

    def near(k, s):
        return [
            remote(
                total.at[s, k, (rings[k].p2 + shift + 4) % 4], nearr.at[s, k, i],
                bs.at[k, s, i], br.at[k, s, i], rings[k].along2(shift),
            )
            for i, shift in enumerate((1, -1))
        ]

    def first(k, s):
        return [
            remote(
                mid.at[s, k, (rings[k].p1 + shift + 4) % 4], firstr.at[s, k, i],
                as_.at[k, s, i], ar.at[k, s, i], rings[k].along1(shift),
            )
            for i, shift in enumerate((1, -1, 2))
        ]

    def zcopy(k, s):
        return remote(zsend.at[s, k], zrecv.at[s, k], zs.at[k, s], zr.at[k, s], device(x, y, target(s), c))

    def flatcross(s):
        return remote(fsend.at[s], frecv.at[s], cs.at[s], cr.at[s], device(x, y, z, 1 - c))

    def flatz(s):
        return remote(
            flat.at[s], flatr.at[s], gs.at[s], gr.at[s], device(x, y, (z + 1 - 2 * (s % 2) + NZ) % NZ, c)
        )

    def flat2():
        return [
            remote(
                flat.at[STEPS - 1, (x + shift + 4) % 4], slabr.at[i], fs.at[i], fr.at[i], rings[0].along2(shift)
            )
            for i, shift in enumerate((1, -1, 2))
        ]

    def flat1():
        return [
            remote(line.at[(y + shift + 4) % 4], liner.at[i], fs.at[3 + i], fr.at[3 + i], rings[0].along1(shift))
            for i, shift in enumerate((1, -1, 2))
        ]

    def product(s, core, store):
        base = target(s) * 512 + core * 128
        rhs = jnp.concatenate(
            [hidden[:, pl.ds(pl.multiple_of(base + y_hi * 256, 128), 128)] for y_hi in range(2)], axis=1
        )
        for part, ref in enumerate((key_ref, value_ref)):
            grads = jnp.dot(ref[...], rhs, preferred_element_type=F32)
            for row in range(4):
                xx = part * 2 + row // 2
                for y_hi in range(2):
                    yy = y_hi * 2 + row % 2
                    lanes = slice(y_hi * 128, (y_hi + 1) * 128)
                    block = grads[row * 128 : row * 128 + 128, lanes]
                    store(0, xx, yy, block[:PART])
                    store(1, yy, xx, block[PART : 2 * PART])
                    store(2, xx, yy, block[2 * PART :])

    def give(s):
        def away(k, i, j, block):
            if k < 2:
                dsend[s, k, i, j] = block.astype(BF)
            else:
                fsend[s, i, j] = block.astype(BF)

        product(s, 1 - c, away)

    def stage0(s):
        def keep(k, i, j, block):
            if k < 2:
                own[s % 4, k, i, j] = block
            else:
                fown[s % 4, i, j] = block

        @pl.when(s > 0)
        def _():
            load(s).wait()
            give(s)

        for k in range(2):
            cross(k, s).start()
        flatcross(s).start()
        product(s, c, keep)

    def stage1(s):
        for k in range(2):
            cross(k, s).wait_recv()
            for place in range(4):
                total[s, k, place] = (own[s % 4, k, place] + drecv[s, k, place].astype(F32)).astype(BF)
            for copy in far(k, s):
                copy.start()

    def stage2(s):
        for k in range(2):
            for copy in far(k, s):
                copy.wait_recv()
            for i, shift in enumerate((1, -1)):
                place = (rings[k].p2 + shift + 4) % 4
                half = slice(2 * i, 2 * i + 2)
                total[s, k, place, half] = (
                    total[s, k, place, half].astype(F32) + farr[s, k, half].astype(F32)
                ).astype(BF)
            for copy in near(k, s):
                copy.start()

    def stage3(s):
        for k in range(2):
            for copy in near(k, s):
                copy.wait_recv()
            mid[s, k] = (
                total[s, k, rings[k].p2].astype(F32) + nearr[s, k, 0].astype(F32) + nearr[s, k, 1].astype(F32)
            ).astype(BF)
            for copy in first(k, s):
                copy.start()

    def stage4(s):
        for k in range(2):
            for copy in first(k, s):
                copy.wait_recv()
            summed = mid[s, k, rings[k].p1].astype(F32)
            for i in range(3):
                summed = summed + firstr[s, k, i].astype(F32)
            last[k] = summed
            zsend[s, k] = summed.astype(BF)

        @pl.when(s < STEPS - 1)
        def _():
            for k in range(2):
                zcopy(k, s).start()

    def chain(s):
        flatcross(s).wait_recv()

        def gathered(extra):
            for place in range(4):
                value = fown[s % 4, place] + frecv[s, place].astype(F32)
                for step in extra:
                    value = value + flatr[step, place].astype(F32)
                flat[s, place] = value.astype(BF)

        @pl.when(s < 2)
        def _():
            gathered(())

        @pl.when((s >= 2) & (s < STEPS - 1))
        def _():
            flatz(s - 2).wait_recv()
            gathered((s - 2,))

        @pl.when(s < STEPS - 1)
        def _():
            flatz(s).start()

        @pl.when(s == STEPS - 1)
        def _():
            flatz(STEPS - 3).wait_recv()
            flatz(STEPS - 2).wait_recv()
            gathered((STEPS - 3, STEPS - 2))
            for copy in flat2():
                copy.start()

    def plane2(s):
        for copy in flat2():
            copy.wait_recv()
        value = flat[STEPS - 1, x].astype(F32)
        for i in range(3):
            value = value + slabr[i].astype(F32)
        line[...] = value.astype(BF)
        for copy in flat1():
            copy.start()

    load(0).wait()
    give(0)
    pl.semaphore_wait(barrier, count)
    pipeline(
        (stage2, REDUCE[2], 0, STEPS),
        (stage1, REDUCE[1], 0, STEPS),
        (stage3, REDUCE[3], 0, STEPS),
        (stage4, REDUCE[4], 0, STEPS),
        (chain, CHAIN, 0, STEPS),
        (plane2, CHAIN + STEPS + 1, 0, 1),
        (stage0, REDUCE[0], 0, STEPS),
    )
    sums = []
    for k in range(2):
        value = last[k]
        for s in range(STEPS - 1):
            zcopy(k, s).wait_recv()
            value = value + zrecv[s, k].astype(F32)
        sums.append(value)
    for copy in flat1():
        copy.wait_recv()
    value = line[y].astype(F32)
    for i in range(3):
        value = value + liner[i].astype(F32)
    sums.append(value)
    t = time_ref[0]
    out_ref[...] = jnp.concatenate(sums, axis=0).T * (2.0 * t * (1.0 - t))

    def drain(s, carry):
        for k in range(2):
            @pl.when(s < STEPS - 1)
            def _():
                zcopy(k, s).wait_send()

            for copy in first(k, s) + near(k, s) + far(k, s) + [cross(k, s)]:
                copy.wait_send()

        @pl.when(s < STEPS - 1)
        def _():
            flatz(s).wait_send()

        flatcross(s).wait_send()
        return carry

    lax.fori_loop(0, STEPS, drain, 0)
    for copy in flat1() + flat2():
        copy.wait_send()


def reduce(key_grad, value_grad, time, hidden):
    vmem = pl.BlockSpec(memory_space=pltpu.VMEM)
    dma = pltpu.SemaphoreType.DMA
    return pl.pallas_call(
        reduce_kernel,
        name="gradient_reduce",
        out_shape=jax.ShapeDtypeStruct((128, 128), F32),
        in_specs=[vmem, vmem, pl.BlockSpec(memory_space=pltpu.SMEM), pl.BlockSpec(memory_space=pl.ANY)],
        out_specs=vmem,
        scratch_shapes=[
            pltpu.VMEM((SEQ, 4096), BF),
            pltpu.VMEM((STEPS, 2, 4, 4, PART, 128), BF),
            pltpu.VMEM((STEPS, 2, 4, 4, PART, 128), BF),
            pltpu.VMEM((4, 2, 4, 4, PART, 128), F32),
            pltpu.VMEM((STEPS, 2, 4, 4, PART, 128), BF),
            pltpu.VMEM((STEPS, 2, 4, PART, 128), BF),
            pltpu.VMEM((STEPS, 2, 2, 4, PART, 128), BF),
            pltpu.VMEM((STEPS, 2, 4, PART, 128), BF),
            pltpu.VMEM((STEPS, 2, 3, PART, 128), BF),
            pltpu.VMEM((STEPS, 2, PART, 128), BF),
            pltpu.VMEM((STEPS, 2, PART, 128), BF),
            pltpu.VMEM((2, PART, 128), F32),
            pltpu.VMEM((STEPS, 4, 4, REST, 128), BF),
            pltpu.VMEM((STEPS, 4, 4, REST, 128), BF),
            pltpu.VMEM((4, 4, 4, REST, 128), F32),
            pltpu.VMEM((STEPS, 4, 4, REST, 128), BF),
            pltpu.VMEM((STEPS, 4, 4, REST, 128), BF),
            pltpu.VMEM((3, 4, REST, 128), BF),
            pltpu.VMEM((4, REST, 128), BF),
            pltpu.VMEM((3, REST, 128), BF),
            dma((2, STEPS)), dma((2, STEPS)),
            dma((2, STEPS, 4)), dma((2, STEPS, 4)),
            dma((2, STEPS, 3)), dma((2, STEPS, 3)),
            dma((2, STEPS)), dma((2, STEPS)),
            dma((STEPS,)), dma((STEPS,)),
            dma((STEPS,)), dma((STEPS,)),
            dma((6,)), dma((6,)),
            dma((STEPS,)),
        ],
        compiler_params=pltpu.CompilerParams(collective_id=1, has_side_effects=True, vmem_limit_bytes=60 * 2**20),
    )(key_grad, value_grad, time, hidden)


def local(hidden, queries, cotangent, point_start, point_mid, point_end, curve_time):
    kv = project(point_start, point_mid, point_end, curve_time, hidden)
    context, key_grad, value_grad = attend(kv, queries, cotangent)
    return context, reduce(key_grad, value_grad, curve_time, hidden)


def solution(mesh):
    return jax.shard_map(
        local,
        mesh=mesh,
        in_specs=(
            P(("dp", "fsdp"), None),
            P(("dp", "fsdp"), None),
            P(("dp", "fsdp"), None),
            P("fsdp", "dp"),
            P("fsdp", "dp"),
            P("fsdp", "dp"),
            P(),
        ),
        out_specs=(P(("dp", "fsdp"), None), P("fsdp", "dp")),
        check_vma=False,
    )
```

```python
import math

import jax
import jax.numpy as jnp
import numpy as np
from jax import lax
from jax.experimental import pallas as pl
from jax.experimental.pallas import tpu as pltpu
from jax.sharding import PartitionSpec as P

KVH = 4
HD = 128
SEQ = 512
BF = jnp.bfloat16
F32 = jnp.float32
NZ = 8
STEPS = 8
GATHER = (0, 2, 4, 6, 7)
REDUCE = (0, 1, 3, 5, 7)
PART = 56
CHAIN = 2
REST = 128 - 2 * PART
MESH = pl.DeviceIdType.MESH
NT = (((1,), (1,)), ((), ()))
TN = (((0,), (0,)), ((), ()))


def coordinates():
    dp = lax.axis_index("dp")
    fsdp = lax.axis_index("fsdp")
    x = dp // 2
    y = (fsdp // 2) % 2 * 2 + dp % 2
    z = fsdp // 4
    c = fsdp % 2
    return x, y, z, c


def device(x, y, z, c):
    return (x * 2 + y % 2, (z * 2 + y // 2) * 2 + c)


def offset(step):
    return (step + 1) // 2 * (2 * (step % 2) - 1)


class Ring:
    def __init__(self, colour, x, y, z, c):
        self.colour = colour
        self.x, self.y, self.z, self.c = x, y, z, c
        self.p1, self.p2 = (y, x) if colour == 0 else (x, y)

    def along1(self, shift):
        if self.colour == 0:
            return device(self.x, (self.y + shift + 4) % 4, self.z, self.c)
        return device((self.x + shift + 4) % 4, self.y, self.z, self.c)

    def along2(self, shift):
        if self.colour == 0:
            return device((self.x + shift + 4) % 4, self.y, self.z, self.c)
        return device(self.x, (self.y + shift + 4) % 4, self.z, self.c)


def remote(src, dst, send, recv, target):
    return pltpu.make_async_remote_copy(
        src_ref=src, dst_ref=dst, send_sem=send, recv_sem=recv, device_id=target, device_id_type=MESH
    )


def greet(x, y, z, c, shifts):
    barrier = pltpu.get_barrier_semaphore()
    peers = [device(x, y, (z + shift) % NZ, c) for shift in shifts]
    peers += [device((x + shift) % 4, y, z, c) for shift in (1, 2, 3)]
    peers += [device(x, (y + shift) % 4, z, c) for shift in (1, 2, 3)]
    peers += [device(x, y, z, 1 - c)]
    for peer in peers:
        pl.semaphore_signal(barrier, inc=1, device_id=peer, device_id_type=MESH)
    return barrier, len(peers)


def pipeline(*stages):
    def body(t, carry):
        for stage, start, first, count in stages:
            @pl.when((t >= start) & (t < start + count))
            def _():
                stage(t - start + first)

        return carry

    lax.fori_loop(0, max(start + count for _, start, _, count in stages), body, 0)


def project_kernel(
    start_ref, mid_ref, end_ref, time_ref, hidden_hbm, out_ref,
    hidden, buf, flat, acc, zs, zr, as_, ar, bs, br, ds_, dr, fs, fr, gs, gr, cs, cr, hsem,
):
    x, y, z, c = coordinates()
    barrier, count = greet(x, y, z, c, (1, NZ - 1))
    load = pltpu.make_async_copy(hidden_hbm, hidden, hsem)
    load.start()
    t = time_ref[0]
    blended = (
        (1.0 - t) ** 2 * start_ref[...].astype(F32)
        + 2.0 * t * (1.0 - t) * mid_ref[...].astype(F32)
        + t**2 * end_ref[...].astype(F32)
    ).astype(BF)
    buf[0, z, c, x, y] = blended[:PART]
    buf[1, z, c, y, x] = blended[PART : 2 * PART]
    flat[z, c, x, y] = blended[2 * PART :]
    acc[...] = jnp.zeros_like(acc)
    rings = [Ring(k, x, y, z, c) for k in range(2)]
    pl.semaphore_wait(barrier, count)

    def zblock(s):
        return (z + offset(s) + NZ) % NZ

    def zcopy(k, s):
        sign = 2 * (s % 2) - 1
        block = buf.at[k, (z + offset(s) - sign + NZ) % NZ, c, rings[k].p2, rings[k].p1]
        return remote(block, block, zs.at[k, s], zr.at[k, s], device(x, y, (z - sign + NZ) % NZ, c))

    def first(k, s):
        block = buf.at[k, zblock(s), c, rings[k].p2, rings[k].p1]
        return [
            remote(block, block, as_.at[k, s, i], ar.at[k, s, i], rings[k].along1(shift))
            for i, shift in enumerate((1, -1, 2))
        ]

    def near(k, s):
        block = buf.at[k, zblock(s), c, rings[k].p2]
        return [
            remote(block, block, bs.at[k, s, i], br.at[k, s, i], rings[k].along2(shift))
            for i, shift in enumerate((1, -1))
        ]

    def far(k, s):
        copies = []
        for i, shift in enumerate((1, -1)):
            block = buf.at[k, zblock(s), c, (rings[k].p2 - shift + 4) % 4, pl.ds(2 * i, 2)]
            copies.append(remote(block, block, bs.at[k, s, 2 + i], br.at[k, s, 2 + i], rings[k].along2(shift)))
        return copies

    def cross(k, s, shift):
        block = buf.at[k, zblock(s), c, (rings[k].p2 + shift + 4) % 4]
        return remote(block, block, ds_.at[k, s, shift + 1], dr.at[k, s, shift + 1], device(x, y, z, 1 - c))

    def flat1():
        block = flat.at[z, c, x, y]
        return [
            remote(block, block, fs.at[i], fr.at[i], rings[0].along1(shift)) for i, shift in enumerate((1, -1, 2))
        ]

    def flat2():
        block = flat.at[z, c, x]
        return [
            remote(block, block, fs.at[3 + i], fr.at[3 + i], rings[0].along2(shift))
            for i, shift in enumerate((1, -1, 2))
        ]

    def flatz(s):
        sign = 2 * (s % 2) - 1
        block = flat.at[(z + offset(s) - sign + NZ) % NZ, c]
        return remote(block, block, gs.at[s], gr.at[s], device(x, y, (z - sign + NZ) % NZ, c))

    def flatcross(s):
        block = flat.at[zblock(s), c]
        return remote(block, block, cs.at[s], cr.at[s], device(x, y, z, 1 - c))

    for s in range(1, 3):
        for k in range(2):
            zcopy(k, s).start()
    for copy in flat1():
        copy.start()
    load.wait()

    def plane1(s):
        for copy in flat1():
            copy.wait_recv()
        for copy in flat2():
            copy.start()

    def plane2(s):
        for copy in flat2():
            copy.wait_recv()
        flatz(1).start()
        flatz(2).start()
        flatcross(0).start()

    def chain(s):
        flatz(s).wait_recv()

        @pl.when(s < STEPS - 2)
        def _():
            flatz(s + 2).start()

        flatcross(s).start()

    def stage0(s):
        @pl.when(s > 0)
        def _():
            for k in range(2):
                zcopy(k, s).wait_recv()

            @pl.when(s < STEPS - 2)
            def _():
                for k in range(2):
                    zcopy(k, s + 2).start()

        for k in range(2):
            for copy in first(k, s):
                copy.start()

    def stage1(s):
        for k in range(2):
            for copy in first(k, s):
                copy.wait_recv()
            for copy in near(k, s):
                copy.start()
            cross(k, s, 0).start()

    def stage2(s):
        for k in range(2):
            for copy in near(k, s):
                copy.wait_recv()
            for copy in far(k, s):
                copy.start()
            cross(k, s, -1).start()
            cross(k, s, 1).start()

    def stage3(s):
        for k in range(2):
            for copy in far(k, s):
                copy.wait_recv()
            cross(k, s, 2).start()

    def stage4(s):
        for k in range(2):
            for shift in range(-1, 3):
                cross(k, s, shift).wait_recv()
        flatcross(s).wait_recv()
        zb = zblock(s)
        lhs = hidden[:, pl.ds(pl.multiple_of(zb * 512, 512), 512)]
        for n in range(4):
            groups = []
            for y_hi in range(2):
                for core in range(2):
                    pair = (y_hi * 2, y_hi * 2 + 1)
                    groups.append(jnp.concatenate([buf[0, zb, core, n, yy] for yy in pair], axis=1))
                    groups.append(jnp.concatenate([buf[1, zb, core, yy, n] for yy in pair], axis=1))
                    groups.append(jnp.concatenate([flat[zb, core, n, yy] for yy in pair], axis=1))
            rhs = jnp.concatenate(groups, axis=0)
            acc[:, n * 256 : (n + 1) * 256] += jnp.dot(lhs, rhs, preferred_element_type=F32)

    pipeline(
        (stage0, GATHER[0], 0, STEPS),
        (stage1, GATHER[1], 0, STEPS),
        (stage2, GATHER[2], 0, STEPS),
        (stage3, GATHER[3], 0, STEPS),
        (plane1, 1, 0, 1),
        (plane2, 3, 0, 1),
        (chain, 6, 1, STEPS - 1),
        (stage4, GATHER[4], 0, STEPS),
    )
    out_ref[...] = acc[...].astype(BF)

    def drain(s, carry):
        for k in range(2):
            @pl.when(s > 0)
            def _():
                zcopy(k, s).wait_send()

            for copy in first(k, s) + near(k, s) + far(k, s):
                copy.wait_send()
            for shift in range(-1, 3):
                cross(k, s, shift).wait_send()

        @pl.when(s > 0)
        def _():
            flatz(s).wait_send()

        flatcross(s).wait_send()
        return carry

    lax.fori_loop(0, STEPS, drain, 0)
    for copy in flat1() + flat2():
        copy.wait_send()


def project(start, mid, end, time, hidden):
    vmem = pl.BlockSpec(memory_space=pltpu.VMEM)
    dma = pltpu.SemaphoreType.DMA
    return pl.pallas_call(
        project_kernel,
        name="gather_project",
        out_shape=jax.ShapeDtypeStruct((SEQ, 1024), BF),
        in_specs=[vmem, vmem, vmem, pl.BlockSpec(memory_space=pltpu.SMEM), pl.BlockSpec(memory_space=pl.ANY)],
        out_specs=vmem,
        scratch_shapes=[
            pltpu.VMEM((SEQ, 4096), BF),
            pltpu.VMEM((2, NZ, 2, 4, 4, PART, 128), BF),
            pltpu.VMEM((NZ, 2, 4, 4, REST, 128), BF),
            pltpu.VMEM((SEQ, 1024), F32),
            dma((2, STEPS)), dma((2, STEPS)),
            dma((2, STEPS, 3)), dma((2, STEPS, 3)),
            dma((2, STEPS, 4)), dma((2, STEPS, 4)),
            dma((2, STEPS, 4)), dma((2, STEPS, 4)),
            dma((6,)), dma((6,)),
            dma((STEPS,)), dma((STEPS,)),
            dma((STEPS,)), dma((STEPS,)),
            dma(()),
        ],
        compiler_params=pltpu.CompilerParams(collective_id=0, has_side_effects=True, vmem_limit_bytes=60 * 2**20),
    )(start, mid, end, time, hidden)


ROWS = 256
SCALE = 1.0 / math.sqrt(HD)
FOLD = SCALE * math.log2(math.e)


def attend_kernel(
    keys_ref, values_ref, query_ref, grad_ref, cos_ref, sin_ref, cost_ref, sint_ref,
    context_ref, key_grad_ref, value_grad_ref, key_acc, value_acc,
):
    raw = keys_ref[...].astype(F32)
    keys = (raw * cos_ref[...] + pltpu.roll(raw, 64, 1) * sin_ref[...]).astype(BF)
    values = values_ref[...]
    key_acc[...] = jnp.zeros_like(key_acc)
    value_acc[...] = jnp.zeros_like(value_acc)
    causal = lax.broadcasted_iota(jnp.int32, (ROWS, ROWS), 0) >= lax.broadcasted_iota(jnp.int32, (ROWS, ROWS), 1)
    causal = jnp.concatenate([causal] * 4, axis=0)
    for tile in range(SEQ // ROWS):
        rows = slice(tile * ROWS, (tile + 1) * ROWS)
        length = (tile + 1) * ROWS
        k_t = keys[:length]
        v_t = values[:length]
        query = jnp.concatenate([query_ref[rows, h * HD : (h + 1) * HD] for h in range(4)], axis=0)
        grad = jnp.concatenate([grad_ref[rows, h * HD : (h + 1) * HD] for h in range(4)], axis=0)
        scores = lax.dot_general(query, k_t, NT, preferred_element_type=F32)
        dprobs = lax.dot_general(grad, v_t, NT, preferred_element_type=F32)
        diagonal = jnp.where(causal, scores[:, length - ROWS :], -1e30)
        scores = diagonal if tile == 0 else jnp.concatenate([scores[:, : length - ROWS], diagonal], axis=1)
        top = jnp.max(scores, axis=-1, keepdims=True)
        weights = jnp.exp2((scores - top) * FOLD)
        probs = weights * (1.0 / jnp.sum(weights, axis=-1, keepdims=True))
        low = probs.astype(BF)
        context = jnp.dot(low, v_t, preferred_element_type=F32)
        for h in range(4):
            context_ref[rows, h * HD : (h + 1) * HD] = context[h * ROWS : (h + 1) * ROWS].astype(BF)
        inner = jnp.sum(context * grad.astype(F32), axis=-1, keepdims=True)
        dscores = (probs * (dprobs - inner)).astype(BF)
        value_acc[:, :length] += lax.dot_general(grad, low, TN, preferred_element_type=F32)
        key_acc[:, :length] += lax.dot_general(query, dscores, TN, preferred_element_type=F32)
    value_grad_ref[...] = value_acc[...].astype(BF)
    first = key_acc[:64] * SCALE
    second = key_acc[64:] * SCALE
    cos = cost_ref[...]
    sin = sint_ref[...]
    key_grad_ref[:64] = (first * cos + second * sin).astype(BF)
    key_grad_ref[64:] = (second * cos - first * sin).astype(BF)


def tables():
    half = HD // 2
    inverse = np.exp(-(2.0 * np.arange(half) / HD) * math.log(500000.0))
    angles = np.arange(SEQ)[:, None] * inverse[None, :]
    cos = np.cos(angles).astype(np.float32)
    sin = np.sin(angles).astype(np.float32)
    return (
        np.concatenate([cos, cos], axis=1),
        np.concatenate([-sin, sin], axis=1),
        np.ascontiguousarray(cos.T),
        np.ascontiguousarray(sin.T),
    )


def attend(kv, queries, cotangent):
    cos, sin, cost, sint = (jnp.asarray(table) for table in tables())
    whole = lambda shape: pl.BlockSpec(shape, lambda j: (0, 0))
    return pl.pallas_call(
        attend_kernel,
        name="attend",
        grid=(KVH,),
        out_shape=(
            jax.ShapeDtypeStruct((SEQ, 2048), BF),
            jax.ShapeDtypeStruct((512, SEQ), BF),
            jax.ShapeDtypeStruct((512, SEQ), BF),
        ),
        in_specs=[
            pl.BlockSpec((SEQ, HD), lambda j: (0, j)),
            pl.BlockSpec((SEQ, HD), lambda j: (0, j + KVH)),
            pl.BlockSpec((SEQ, 512), lambda j: (0, j)),
            pl.BlockSpec((SEQ, 512), lambda j: (0, j)),
            whole((SEQ, HD)), whole((SEQ, HD)), whole((HD // 2, SEQ)), whole((HD // 2, SEQ)),
        ],
        out_specs=(
            pl.BlockSpec((SEQ, 512), lambda j: (0, j)),
            pl.BlockSpec((HD, SEQ), lambda j: (j, 0)),
            pl.BlockSpec((HD, SEQ), lambda j: (j, 0)),
        ),
        scratch_shapes=[pltpu.VMEM((HD, SEQ), F32), pltpu.VMEM((HD, SEQ), F32)],
        compiler_params=pltpu.CompilerParams(vmem_limit_bytes=60 * 2**20),
    )(kv, kv, queries, cotangent, cos, sin, cost, sint)


def reduce_kernel(
    key_ref, value_ref, time_ref, hidden_hbm, out_ref,
    hidden, dsend, drecv, own, total, farr, nearr, mid, firstr, zsend, zrecv, last,
    fsend, frecv, fown, flat, flatr, slabr, line, liner,
    ds_, dr, bs, br, as_, ar, zs, zr, cs, cr, gs, gr, fs, fr, hsem,
):
    x, y, z, c = coordinates()
    barrier, count = greet(x, y, z, c, range(1, NZ))
    rings = [Ring(k, x, y, z, c) for k in range(2)]

    def target(s):
        return (z + offset(7 - s) + NZ) % NZ

    def load(s):
        columns = pl.ds(pl.multiple_of(target(s) * 512, 512), 512)
        return pltpu.make_async_copy(hidden_hbm.at[:, columns], hidden.at[:, columns], hsem.at[s])

    for s in range(STEPS):
        load(s).start()

    def cross(k, s):
        return remote(dsend.at[s, k], drecv.at[s, k], ds_.at[k, s], dr.at[k, s], device(x, y, z, 1 - c))

    def far(k, s):
        copies = []
        for i, shift in enumerate((1, -1)):
            half = pl.ds(2 * i, 2)
            source = total.at[s, k, (rings[k].p2 + 2) % 4, half]
            copies.append(
                remote(source, farr.at[s, k, half], bs.at[k, s, 2 + i], br.at[k, s, 2 + i], rings[k].along2(shift))
            )
        return copies

    def near(k, s):
        return [
            remote(
                total.at[s, k, (rings[k].p2 + shift + 4) % 4], nearr.at[s, k, i],
                bs.at[k, s, i], br.at[k, s, i], rings[k].along2(shift),
            )
            for i, shift in enumerate((1, -1))
        ]

    def first(k, s):
        return [
            remote(
                mid.at[s, k, (rings[k].p1 + shift + 4) % 4], firstr.at[s, k, i],
                as_.at[k, s, i], ar.at[k, s, i], rings[k].along1(shift),
            )
            for i, shift in enumerate((1, -1, 2))
        ]

    def zcopy(k, s):
        return remote(zsend.at[s, k], zrecv.at[s, k], zs.at[k, s], zr.at[k, s], device(x, y, target(s), c))

    def flatcross(s):
        return remote(fsend.at[s], frecv.at[s], cs.at[s], cr.at[s], device(x, y, z, 1 - c))

    def flatz(s):
        return remote(
            flat.at[s], flatr.at[s], gs.at[s], gr.at[s], device(x, y, (z + 1 - 2 * (s % 2) + NZ) % NZ, c)
        )

    def flat2():
        return [
            remote(
                flat.at[STEPS - 1, (x + shift + 4) % 4], slabr.at[i], fs.at[i], fr.at[i], rings[0].along2(shift)
            )
            for i, shift in enumerate((1, -1, 2))
        ]

    def flat1():
        return [
            remote(line.at[(y + shift + 4) % 4], liner.at[i], fs.at[3 + i], fr.at[3 + i], rings[0].along1(shift))
            for i, shift in enumerate((1, -1, 2))
        ]

    def product(s, core, store):
        base = target(s) * 512 + core * 128
        rhs = jnp.concatenate(
            [hidden[:, pl.ds(pl.multiple_of(base + y_hi * 256, 128), 128)] for y_hi in range(2)], axis=1
        )
        for part, ref in enumerate((key_ref, value_ref)):
            grads = jnp.dot(ref[...], rhs, preferred_element_type=F32)
            for row in range(4):
                xx = part * 2 + row // 2
                for y_hi in range(2):
                    yy = y_hi * 2 + row % 2
                    lanes = slice(y_hi * 128, (y_hi + 1) * 128)
                    block = grads[row * 128 : row * 128 + 128, lanes]
                    store(0, xx, yy, block[:PART])
                    store(1, yy, xx, block[PART : 2 * PART])
                    store(2, xx, yy, block[2 * PART :])

    def give(s):
        def away(k, i, j, block):
            if k < 2:
                dsend[s, k, i, j] = block.astype(BF)
            else:
                fsend[s, i, j] = block.astype(BF)

        product(s, 1 - c, away)

    def stage0(s):
        def keep(k, i, j, block):
            if k < 2:
                own[s % 4, k, i, j] = block
            else:
                fown[s % 4, i, j] = block

        @pl.when(s > 0)
        def _():
            load(s).wait()
            give(s)

        for k in range(2):
            cross(k, s).start()
        flatcross(s).start()
        product(s, c, keep)

    def stage1(s):
        for k in range(2):
            cross(k, s).wait_recv()
            for place in range(4):
                total[s, k, place] = (own[s % 4, k, place] + drecv[s, k, place].astype(F32)).astype(BF)
            for copy in far(k, s):
                copy.start()

    def stage2(s):
        for k in range(2):
            for copy in far(k, s):
                copy.wait_recv()
            for i, shift in enumerate((1, -1)):
                place = (rings[k].p2 + shift + 4) % 4
                half = slice(2 * i, 2 * i + 2)
                total[s, k, place, half] = (
                    total[s, k, place, half].astype(F32) + farr[s, k, half].astype(F32)
                ).astype(BF)
            for copy in near(k, s):
                copy.start()

    def stage3(s):
        for k in range(2):
            for copy in near(k, s):
                copy.wait_recv()
            mid[s, k] = (
                total[s, k, rings[k].p2].astype(F32) + nearr[s, k, 0].astype(F32) + nearr[s, k, 1].astype(F32)
            ).astype(BF)
            for copy in first(k, s):
                copy.start()

    def stage4(s):
        for k in range(2):
            for copy in first(k, s):
                copy.wait_recv()
            summed = mid[s, k, rings[k].p1].astype(F32)
            for i in range(3):
                summed = summed + firstr[s, k, i].astype(F32)
            last[k] = summed
            zsend[s, k] = summed.astype(BF)

        @pl.when(s < STEPS - 1)
        def _():
            for k in range(2):
                zcopy(k, s).start()

    def chain(s):
        flatcross(s).wait_recv()

        def gathered(extra):
            for place in range(4):
                value = fown[s % 4, place] + frecv[s, place].astype(F32)
                for step in extra:
                    value = value + flatr[step, place].astype(F32)
                flat[s, place] = value.astype(BF)

        @pl.when(s < 2)
        def _():
            gathered(())

        @pl.when((s >= 2) & (s < STEPS - 1))
        def _():
            flatz(s - 2).wait_recv()
            gathered((s - 2,))

        @pl.when(s < STEPS - 1)
        def _():
            flatz(s).start()

        @pl.when(s == STEPS - 1)
        def _():
            flatz(STEPS - 3).wait_recv()
            flatz(STEPS - 2).wait_recv()
            gathered((STEPS - 3, STEPS - 2))
            for copy in flat2():
                copy.start()

    def plane2(s):
        for copy in flat2():
            copy.wait_recv()
        value = flat[STEPS - 1, x].astype(F32)
        for i in range(3):
            value = value + slabr[i].astype(F32)
        line[...] = value.astype(BF)
        for copy in flat1():
            copy.start()

    load(0).wait()
    give(0)
    pl.semaphore_wait(barrier, count)
    pipeline(
        (stage2, REDUCE[2], 0, STEPS),
        (stage1, REDUCE[1], 0, STEPS),
        (stage3, REDUCE[3], 0, STEPS),
        (stage4, REDUCE[4], 0, STEPS),
        (chain, CHAIN, 0, STEPS),
        (plane2, CHAIN + STEPS + 1, 0, 1),
        (stage0, REDUCE[0], 0, STEPS),
    )
    sums = []
    for k in range(2):
        value = last[k]
        for s in range(STEPS - 1):
            zcopy(k, s).wait_recv()
            value = value + zrecv[s, k].astype(F32)
        sums.append(value)
    for copy in flat1():
        copy.wait_recv()
    value = line[y].astype(F32)
    for i in range(3):
        value = value + liner[i].astype(F32)
    sums.append(value)
    t = time_ref[0]
    out_ref[...] = jnp.concatenate(sums, axis=0).T * (2.0 * t * (1.0 - t))

    def drain(s, carry):
        for k in range(2):
            @pl.when(s < STEPS - 1)
            def _():
                zcopy(k, s).wait_send()

            for copy in first(k, s) + near(k, s) + far(k, s) + [cross(k, s)]:
                copy.wait_send()

        @pl.when(s < STEPS - 1)
        def _():
            flatz(s).wait_send()

        flatcross(s).wait_send()
        return carry

    lax.fori_loop(0, STEPS, drain, 0)
    for copy in flat1() + flat2():
        copy.wait_send()


def reduce(key_grad, value_grad, time, hidden):
    vmem = pl.BlockSpec(memory_space=pltpu.VMEM)
    dma = pltpu.SemaphoreType.DMA
    return pl.pallas_call(
        reduce_kernel,
        name="gradient_reduce",
        out_shape=jax.ShapeDtypeStruct((128, 128), F32),
        in_specs=[vmem, vmem, pl.BlockSpec(memory_space=pltpu.SMEM), pl.BlockSpec(memory_space=pl.ANY)],
        out_specs=vmem,
        scratch_shapes=[
            pltpu.VMEM((SEQ, 4096), BF),
            pltpu.VMEM((STEPS, 2, 4, 4, PART, 128), BF),
            pltpu.VMEM((STEPS, 2, 4, 4, PART, 128), BF),
            pltpu.VMEM((4, 2, 4, 4, PART, 128), F32),
            pltpu.VMEM((STEPS, 2, 4, 4, PART, 128), BF),
            pltpu.VMEM((STEPS, 2, 4, PART, 128), BF),
            pltpu.VMEM((STEPS, 2, 2, 4, PART, 128), BF),
            pltpu.VMEM((STEPS, 2, 4, PART, 128), BF),
            pltpu.VMEM((STEPS, 2, 3, PART, 128), BF),
            pltpu.VMEM((STEPS, 2, PART, 128), BF),
            pltpu.VMEM((STEPS, 2, PART, 128), BF),
            pltpu.VMEM((2, PART, 128), F32),
            pltpu.VMEM((STEPS, 4, 4, REST, 128), BF),
            pltpu.VMEM((STEPS, 4, 4, REST, 128), BF),
            pltpu.VMEM((4, 4, 4, REST, 128), F32),
            pltpu.VMEM((STEPS, 4, 4, REST, 128), BF),
            pltpu.VMEM((STEPS, 4, 4, REST, 128), BF),
            pltpu.VMEM((3, 4, REST, 128), BF),
            pltpu.VMEM((4, REST, 128), BF),
            pltpu.VMEM((3, REST, 128), BF),
            dma((2, STEPS)), dma((2, STEPS)),
            dma((2, STEPS, 4)), dma((2, STEPS, 4)),
            dma((2, STEPS, 3)), dma((2, STEPS, 3)),
            dma((2, STEPS)), dma((2, STEPS)),
            dma((STEPS,)), dma((STEPS,)),
            dma((STEPS,)), dma((STEPS,)),
            dma((6,)), dma((6,)),
            dma((STEPS,)),
        ],
        compiler_params=pltpu.CompilerParams(collective_id=1, has_side_effects=True, vmem_limit_bytes=60 * 2**20),
    )(key_grad, value_grad, time, hidden)


def local(hidden, queries, cotangent, point_start, point_mid, point_end, curve_time):
    kv = project(point_start, point_mid, point_end, curve_time, hidden)
    context, key_grad, value_grad = attend(kv, queries, cotangent)
    return context, reduce(key_grad, value_grad, curve_time, hidden)


def solution(mesh):
    return jax.shard_map(
        local,
        mesh=mesh,
        in_specs=(
            P(("dp", "fsdp"), None),
            P(("dp", "fsdp"), None),
            P(("dp", "fsdp"), None),
            P("fsdp", "dp"),
            P("fsdp", "dp"),
            P("fsdp", "dp"),
            P(),
        ),
        out_specs=(P(("dp", "fsdp"), None), P("fsdp", "dp")),
        check_vma=False,
    )
```

```python
import math

import jax
import jax.numpy as jnp
import numpy as np
from jax import lax
from jax.experimental import pallas as pl
from jax.experimental.pallas import tpu as pltpu
from jax.sharding import PartitionSpec as P

KVH = 4
HD = 128
SEQ = 512
BF = jnp.bfloat16
F32 = jnp.float32
NZ = 8
STEPS = 8
GATHER = (0, 2, 4, 6, 7)
REDUCE = (0, 1, 3, 5, 7)
PART = 56
CHAIN = 2
REST = 128 - 2 * PART
MESH = pl.DeviceIdType.MESH
NT = (((1,), (1,)), ((), ()))
TN = (((0,), (0,)), ((), ()))


def coordinates():
    dp = lax.axis_index("dp")
    fsdp = lax.axis_index("fsdp")
    x = dp // 2
    y = (fsdp // 2) % 2 * 2 + dp % 2
    z = fsdp // 4
    c = fsdp % 2
    return x, y, z, c


def device(x, y, z, c):
    return (x * 2 + y % 2, (z * 2 + y // 2) * 2 + c)


def offset(step):
    return (step + 1) // 2 * (2 * (step % 2) - 1)


class Ring:
    def __init__(self, colour, x, y, z, c):
        self.colour = colour
        self.x, self.y, self.z, self.c = x, y, z, c
        self.p1, self.p2 = (y, x) if colour == 0 else (x, y)

    def along1(self, shift):
        if self.colour == 0:
            return device(self.x, (self.y + shift + 4) % 4, self.z, self.c)
        return device((self.x + shift + 4) % 4, self.y, self.z, self.c)

    def along2(self, shift):
        if self.colour == 0:
            return device((self.x + shift + 4) % 4, self.y, self.z, self.c)
        return device(self.x, (self.y + shift + 4) % 4, self.z, self.c)


def remote(src, dst, send, recv, target):
    return pltpu.make_async_remote_copy(
        src_ref=src, dst_ref=dst, send_sem=send, recv_sem=recv, device_id=target, device_id_type=MESH
    )


def greet(x, y, z, c, shifts):
    barrier = pltpu.get_barrier_semaphore()
    peers = [device(x, y, (z + shift) % NZ, c) for shift in shifts]
    peers += [device((x + shift) % 4, y, z, c) for shift in (1, 2, 3)]
    peers += [device(x, (y + shift) % 4, z, c) for shift in (1, 2, 3)]
    peers += [device(x, y, z, 1 - c)]
    for peer in peers:
        pl.semaphore_signal(barrier, inc=1, device_id=peer, device_id_type=MESH)
    return barrier, len(peers)


def pipeline(*stages):
    def body(t, carry):
        for stage, start, first, count in stages:
            @pl.when((t >= start) & (t < start + count))
            def _():
                stage(t - start + first)

        return carry

    lax.fori_loop(0, max(start + count for _, start, _, count in stages), body, 0)


def project_kernel(
    start_ref, mid_ref, end_ref, time_ref, hidden_hbm, out_ref,
    hidden, buf, flat, acc, zs, zr, as_, ar, bs, br, ds_, dr, fs, fr, gs, gr, cs, cr, hsem,
):
    x, y, z, c = coordinates()
    barrier, count = greet(x, y, z, c, (1, NZ - 1))
    load = pltpu.make_async_copy(hidden_hbm, hidden, hsem)
    load.start()
    t = time_ref[0]
    blended = (
        (1.0 - t) ** 2 * start_ref[...].astype(F32)
        + 2.0 * t * (1.0 - t) * mid_ref[...].astype(F32)
        + t**2 * end_ref[...].astype(F32)
    ).astype(BF)
    buf[0, z, c, x, y] = blended[:PART]
    buf[1, z, c, y, x] = blended[PART : 2 * PART]
    flat[z, c, x, y] = blended[2 * PART :]
    acc[...] = jnp.zeros_like(acc)
    rings = [Ring(k, x, y, z, c) for k in range(2)]
    pl.semaphore_wait(barrier, count)

    def zblock(s):
        return (z + offset(s) + NZ) % NZ

    def zcopy(k, s):
        sign = 2 * (s % 2) - 1
        block = buf.at[k, (z + offset(s) - sign + NZ) % NZ, c, rings[k].p2, rings[k].p1]
        return remote(block, block, zs.at[k, s], zr.at[k, s], device(x, y, (z - sign + NZ) % NZ, c))

    def first(k, s):
        block = buf.at[k, zblock(s), c, rings[k].p2, rings[k].p1]
        return [
            remote(block, block, as_.at[k, s, i], ar.at[k, s, i], rings[k].along1(shift))
            for i, shift in enumerate((1, -1, 2))
        ]

    def near(k, s):
        block = buf.at[k, zblock(s), c, rings[k].p2]
        return [
            remote(block, block, bs.at[k, s, i], br.at[k, s, i], rings[k].along2(shift))
            for i, shift in enumerate((1, -1))
        ]

    def far(k, s):
        copies = []
        for i, shift in enumerate((1, -1)):
            block = buf.at[k, zblock(s), c, (rings[k].p2 - shift + 4) % 4, pl.ds(2 * i, 2)]
            copies.append(remote(block, block, bs.at[k, s, 2 + i], br.at[k, s, 2 + i], rings[k].along2(shift)))
        return copies

    def cross(k, s):
        block = buf.at[k, zblock(s), c]
        return remote(block, block, ds_.at[k, s], dr.at[k, s], device(x, y, z, 1 - c))

    def flat1():
        block = flat.at[z, c, x, y]
        return [
            remote(block, block, fs.at[i], fr.at[i], rings[0].along1(shift)) for i, shift in enumerate((1, -1, 2))
        ]

    def flat2():
        block = flat.at[z, c, x]
        return [
            remote(block, block, fs.at[3 + i], fr.at[3 + i], rings[0].along2(shift))
            for i, shift in enumerate((1, -1, 2))
        ]

    def flatz(s):
        sign = 2 * (s % 2) - 1
        block = flat.at[(z + offset(s) - sign + NZ) % NZ, c]
        return remote(block, block, gs.at[s], gr.at[s], device(x, y, (z - sign + NZ) % NZ, c))

    def flatcross(s):
        block = flat.at[zblock(s), c]
        return remote(block, block, cs.at[s], cr.at[s], device(x, y, z, 1 - c))

    for s in range(1, 3):
        for k in range(2):
            zcopy(k, s).start()
    for copy in flat1():
        copy.start()
    load.wait()

    def plane1(s):
        for copy in flat1():
            copy.wait_recv()
        for copy in flat2():
            copy.start()

    def plane2(s):
        for copy in flat2():
            copy.wait_recv()
        flatz(1).start()
        flatz(2).start()
        flatcross(0).start()

    def chain(s):
        flatz(s).wait_recv()

        @pl.when(s < STEPS - 2)
        def _():
            flatz(s + 2).start()

        flatcross(s).start()

    def stage0(s):
        @pl.when(s > 0)
        def _():
            for k in range(2):
                zcopy(k, s).wait_recv()

            @pl.when(s < STEPS - 2)
            def _():
                for k in range(2):
                    zcopy(k, s + 2).start()

        for k in range(2):
            for copy in first(k, s):
                copy.start()

    def stage1(s):
        for k in range(2):
            for copy in first(k, s):
                copy.wait_recv()
            for copy in near(k, s):
                copy.start()

    def stage2(s):
        for k in range(2):
            for copy in near(k, s):
                copy.wait_recv()
            for copy in far(k, s):
                copy.start()

    def stage3(s):
        for k in range(2):
            for copy in far(k, s):
                copy.wait_recv()
            cross(k, s).start()

    def stage4(s):
        for k in range(2):
            cross(k, s).wait_recv()
        flatcross(s).wait_recv()
        zb = zblock(s)
        lhs = hidden[:, pl.ds(pl.multiple_of(zb * 512, 512), 512)]
        for n in range(4):
            groups = []
            for y_hi in range(2):
                for core in range(2):
                    pair = (y_hi * 2, y_hi * 2 + 1)
                    groups.append(jnp.concatenate([buf[0, zb, core, n, yy] for yy in pair], axis=1))
                    groups.append(jnp.concatenate([buf[1, zb, core, yy, n] for yy in pair], axis=1))
                    groups.append(jnp.concatenate([flat[zb, core, n, yy] for yy in pair], axis=1))
            rhs = jnp.concatenate(groups, axis=0)
            acc[:, n * 256 : (n + 1) * 256] += jnp.dot(lhs, rhs, preferred_element_type=F32)

    pipeline(
        (stage0, GATHER[0], 0, STEPS),
        (stage1, GATHER[1], 0, STEPS),
        (stage2, GATHER[2], 0, STEPS),
        (stage3, GATHER[3], 0, STEPS),
        (plane1, 1, 0, 1),
        (plane2, 3, 0, 1),
        (chain, 6, 1, STEPS - 1),
        (stage4, GATHER[4], 0, STEPS),
    )
    out_ref[...] = acc[...].astype(BF)

    def drain(s, carry):
        for k in range(2):
            @pl.when(s > 0)
            def _():
                zcopy(k, s).wait_send()

            for copy in first(k, s) + near(k, s) + far(k, s) + [cross(k, s)]:
                copy.wait_send()

        @pl.when(s > 0)
        def _():
            flatz(s).wait_send()

        flatcross(s).wait_send()
        return carry

    lax.fori_loop(0, STEPS, drain, 0)
    for copy in flat1() + flat2():
        copy.wait_send()


def project(start, mid, end, time, hidden):
    vmem = pl.BlockSpec(memory_space=pltpu.VMEM)
    dma = pltpu.SemaphoreType.DMA
    return pl.pallas_call(
        project_kernel,
        name="gather_project",
        out_shape=jax.ShapeDtypeStruct((SEQ, 1024), BF),
        in_specs=[vmem, vmem, vmem, pl.BlockSpec(memory_space=pltpu.SMEM), pl.BlockSpec(memory_space=pl.ANY)],
        out_specs=vmem,
        scratch_shapes=[
            pltpu.VMEM((SEQ, 4096), BF),
            pltpu.VMEM((2, NZ, 2, 4, 4, PART, 128), BF),
            pltpu.VMEM((NZ, 2, 4, 4, REST, 128), BF),
            pltpu.VMEM((SEQ, 1024), F32),
            dma((2, STEPS)), dma((2, STEPS)),
            dma((2, STEPS, 3)), dma((2, STEPS, 3)),
            dma((2, STEPS, 4)), dma((2, STEPS, 4)),
            dma((2, STEPS)), dma((2, STEPS)),
            dma((6,)), dma((6,)),
            dma((STEPS,)), dma((STEPS,)),
            dma((STEPS,)), dma((STEPS,)),
            dma(()),
        ],
        compiler_params=pltpu.CompilerParams(collective_id=0, has_side_effects=True, vmem_limit_bytes=60 * 2**20),
    )(start, mid, end, time, hidden)


ROWS = 256
SCALE = 1.0 / math.sqrt(HD)
FOLD = SCALE * math.log2(math.e)


def attend_kernel(
    keys_ref, values_ref, query_ref, grad_ref, cos_ref, sin_ref, cost_ref, sint_ref,
    context_ref, key_grad_ref, value_grad_ref, key_acc, value_acc,
):
    raw = keys_ref[...].astype(F32)
    keys = (raw * cos_ref[...] + pltpu.roll(raw, 64, 1) * sin_ref[...]).astype(BF)
    values = values_ref[...]
    key_acc[...] = jnp.zeros_like(key_acc)
    value_acc[...] = jnp.zeros_like(value_acc)
    causal = lax.broadcasted_iota(jnp.int32, (ROWS, ROWS), 0) >= lax.broadcasted_iota(jnp.int32, (ROWS, ROWS), 1)
    causal = jnp.concatenate([causal] * 4, axis=0)
    for tile in range(SEQ // ROWS):
        rows = slice(tile * ROWS, (tile + 1) * ROWS)
        length = (tile + 1) * ROWS
        k_t = keys[:length]
        v_t = values[:length]
        query = jnp.concatenate([query_ref[rows, h * HD : (h + 1) * HD] for h in range(4)], axis=0)
        grad = jnp.concatenate([grad_ref[rows, h * HD : (h + 1) * HD] for h in range(4)], axis=0)
        scores = lax.dot_general(query, k_t, NT, preferred_element_type=F32)
        diagonal = jnp.where(causal, scores[:, length - ROWS :], -1e30)
        scores = diagonal if tile == 0 else jnp.concatenate([scores[:, : length - ROWS], diagonal], axis=1)
        top = jnp.max(scores, axis=-1, keepdims=True)
        weights = jnp.exp2((scores - top) * FOLD)
        low = weights.astype(BF)
        scale = 1.0 / jnp.sum(weights, axis=-1, keepdims=True)
        context = jnp.dot(low, v_t, preferred_element_type=F32) * scale
        for h in range(4):
            context_ref[rows, h * HD : (h + 1) * HD] = context[h * ROWS : (h + 1) * ROWS].astype(BF)
        grad = (grad.astype(F32) * scale).astype(BF)
        dprobs = lax.dot_general(grad, v_t, NT, preferred_element_type=F32)
        inner = jnp.sum(context * grad.astype(F32), axis=-1, keepdims=True)
        dscores = (weights * (dprobs - inner)).astype(BF)
        value_acc[:, :length] += lax.dot_general(grad, low, TN, preferred_element_type=F32)
        key_acc[:, :length] += lax.dot_general(query, dscores, TN, preferred_element_type=F32)
    value_grad_ref[...] = value_acc[...].astype(BF)
    first = key_acc[:64] * SCALE
    second = key_acc[64:] * SCALE
    cos = cost_ref[...]
    sin = sint_ref[...]
    key_grad_ref[:64] = (first * cos + second * sin).astype(BF)
    key_grad_ref[64:] = (second * cos - first * sin).astype(BF)


def tables():
    half = HD // 2
    inverse = np.exp(-(2.0 * np.arange(half) / HD) * math.log(500000.0))
    angles = np.arange(SEQ)[:, None] * inverse[None, :]
    cos = np.cos(angles).astype(np.float32)
    sin = np.sin(angles).astype(np.float32)
    return (
        np.concatenate([cos, cos], axis=1),
        np.concatenate([-sin, sin], axis=1),
        np.ascontiguousarray(cos.T),
        np.ascontiguousarray(sin.T),
    )


def attend(kv, queries, cotangent):
    cos, sin, cost, sint = (jnp.asarray(table) for table in tables())
    whole = lambda shape: pl.BlockSpec(shape, lambda j: (0, 0))
    return pl.pallas_call(
        attend_kernel,
        name="attend",
        grid=(KVH,),
        out_shape=(
            jax.ShapeDtypeStruct((SEQ, 2048), BF),
            jax.ShapeDtypeStruct((512, SEQ), BF),
            jax.ShapeDtypeStruct((512, SEQ), BF),
        ),
        in_specs=[
            pl.BlockSpec((SEQ, HD), lambda j: (0, j)),
            pl.BlockSpec((SEQ, HD), lambda j: (0, j + KVH)),
            pl.BlockSpec((SEQ, 512), lambda j: (0, j)),
            pl.BlockSpec((SEQ, 512), lambda j: (0, j)),
            whole((SEQ, HD)), whole((SEQ, HD)), whole((HD // 2, SEQ)), whole((HD // 2, SEQ)),
        ],
        out_specs=(
            pl.BlockSpec((SEQ, 512), lambda j: (0, j)),
            pl.BlockSpec((HD, SEQ), lambda j: (j, 0)),
            pl.BlockSpec((HD, SEQ), lambda j: (j, 0)),
        ),
        scratch_shapes=[pltpu.VMEM((HD, SEQ), F32), pltpu.VMEM((HD, SEQ), F32)],
        compiler_params=pltpu.CompilerParams(vmem_limit_bytes=60 * 2**20),
    )(kv, kv, queries, cotangent, cos, sin, cost, sint)


def reduce_kernel(
    key_ref, value_ref, time_ref, hidden_hbm, out_ref,
    hidden, dsend, drecv, own, total, farr, nearr, mid, firstr, zsend, zrecv, last,
    fsend, frecv, fown, flat, flatr, slabr, line, liner,
    ds_, dr, bs, br, as_, ar, zs, zr, cs, cr, gs, gr, fs, fr, hsem,
):
    x, y, z, c = coordinates()
    barrier, count = greet(x, y, z, c, range(1, NZ))
    rings = [Ring(k, x, y, z, c) for k in range(2)]

    def target(s):
        return (z + offset(7 - s) + NZ) % NZ

    def load(s):
        columns = pl.ds(pl.multiple_of(target(s) * 512, 512), 512)
        return pltpu.make_async_copy(hidden_hbm.at[:, columns], hidden.at[:, columns], hsem.at[s])

    for s in range(STEPS):
        load(s).start()

    def cross(k, s):
        return remote(dsend.at[s, k], drecv.at[s, k], ds_.at[k, s], dr.at[k, s], device(x, y, z, 1 - c))

    def far(k, s):
        copies = []
        for i, shift in enumerate((1, -1)):
            half = pl.ds(2 * i, 2)
            source = total.at[s, k, (rings[k].p2 + 2) % 4, half]
            copies.append(
                remote(source, farr.at[s, k, half], bs.at[k, s, 2 + i], br.at[k, s, 2 + i], rings[k].along2(shift))
            )
        return copies

    def near(k, s):
        return [
            remote(
                total.at[s, k, (rings[k].p2 + shift + 4) % 4], nearr.at[s, k, i],
                bs.at[k, s, i], br.at[k, s, i], rings[k].along2(shift),
            )
            for i, shift in enumerate((1, -1))
        ]

    def first(k, s):
        return [
            remote(
                mid.at[s, k, (rings[k].p1 + shift + 4) % 4], firstr.at[s, k, i],
                as_.at[k, s, i], ar.at[k, s, i], rings[k].along1(shift),
            )
            for i, shift in enumerate((1, -1, 2))
        ]

    def zcopy(k, s):
        return remote(zsend.at[s, k], zrecv.at[s, k], zs.at[k, s], zr.at[k, s], device(x, y, target(s), c))

    def flatcross(s):
        return remote(fsend.at[s], frecv.at[s], cs.at[s], cr.at[s], device(x, y, z, 1 - c))

    def flatz(s):
        return remote(
            flat.at[s], flatr.at[s], gs.at[s], gr.at[s], device(x, y, (z + 1 - 2 * (s % 2) + NZ) % NZ, c)
        )

    def flat2():
        return [
            remote(
                flat.at[STEPS - 1, (x + shift + 4) % 4], slabr.at[i], fs.at[i], fr.at[i], rings[0].along2(shift)
            )
            for i, shift in enumerate((1, -1, 2))
        ]

    def flat1():
        return [
            remote(line.at[(y + shift + 4) % 4], liner.at[i], fs.at[3 + i], fr.at[3 + i], rings[0].along1(shift))
            for i, shift in enumerate((1, -1, 2))
        ]

    def product(s, core, store):
        base = target(s) * 512 + core * 128
        rhs = jnp.concatenate(
            [hidden[:, pl.ds(pl.multiple_of(base + y_hi * 256, 128), 128)] for y_hi in range(2)], axis=1
        )
        for part, ref in enumerate((key_ref, value_ref)):
            grads = jnp.dot(ref[...], rhs, preferred_element_type=F32)
            for row in range(4):
                xx = part * 2 + row // 2
                for y_hi in range(2):
                    yy = y_hi * 2 + row % 2
                    lanes = slice(y_hi * 128, (y_hi + 1) * 128)
                    block = grads[row * 128 : row * 128 + 128, lanes]
                    store(0, xx, yy, block[:PART])
                    store(1, yy, xx, block[PART : 2 * PART])
                    store(2, xx, yy, block[2 * PART :])

    def give(s):
        def away(k, i, j, block):
            if k < 2:
                dsend[s, k, i, j] = block.astype(BF)
            else:
                fsend[s, i, j] = block.astype(BF)

        product(s, 1 - c, away)

    def stage0(s):
        def keep(k, i, j, block):
            if k < 2:
                own[s % 4, k, i, j] = block
            else:
                fown[s % 4, i, j] = block

        @pl.when(s > 0)
        def _():
            load(s).wait()
            give(s)

        for k in range(2):
            cross(k, s).start()
        flatcross(s).start()
        product(s, c, keep)

    def stage1(s):
        for k in range(2):
            cross(k, s).wait_recv()
            for place in range(4):
                total[s, k, place] = (own[s % 4, k, place] + drecv[s, k, place].astype(F32)).astype(BF)
            for copy in far(k, s):
                copy.start()

    def stage2(s):
        for k in range(2):
            for copy in far(k, s):
                copy.wait_recv()
            for i, shift in enumerate((1, -1)):
                place = (rings[k].p2 + shift + 4) % 4
                half = slice(2 * i, 2 * i + 2)
                total[s, k, place, half] = (
                    total[s, k, place, half].astype(F32) + farr[s, k, half].astype(F32)
                ).astype(BF)
            for copy in near(k, s):
                copy.start()

    def stage3(s):
        for k in range(2):
            for copy in near(k, s):
                copy.wait_recv()
            mid[s, k] = (
                total[s, k, rings[k].p2].astype(F32) + nearr[s, k, 0].astype(F32) + nearr[s, k, 1].astype(F32)
            ).astype(BF)
            for copy in first(k, s):
                copy.start()

    def stage4(s):
        for k in range(2):
            for copy in first(k, s):
                copy.wait_recv()
            summed = mid[s, k, rings[k].p1].astype(F32)
            for i in range(3):
                summed = summed + firstr[s, k, i].astype(F32)
            last[k] = summed
            zsend[s, k] = summed.astype(BF)

        @pl.when(s < STEPS - 1)
        def _():
            for k in range(2):
                zcopy(k, s).start()

    def chain(s):
        flatcross(s).wait_recv()

        def gathered(extra):
            for place in range(4):
                value = fown[s % 4, place] + frecv[s, place].astype(F32)
                for step in extra:
                    value = value + flatr[step, place].astype(F32)
                flat[s, place] = value.astype(BF)

        @pl.when(s < 2)
        def _():
            gathered(())

        @pl.when((s >= 2) & (s < STEPS - 1))
        def _():
            flatz(s - 2).wait_recv()
            gathered((s - 2,))

        @pl.when(s < STEPS - 1)
        def _():
            flatz(s).start()

        @pl.when(s == STEPS - 1)
        def _():
            flatz(STEPS - 3).wait_recv()
            flatz(STEPS - 2).wait_recv()
            gathered((STEPS - 3, STEPS - 2))
            for copy in flat2():
                copy.start()

    def plane2(s):
        for copy in flat2():
            copy.wait_recv()
        value = flat[STEPS - 1, x].astype(F32)
        for i in range(3):
            value = value + slabr[i].astype(F32)
        line[...] = value.astype(BF)
        for copy in flat1():
            copy.start()

    load(0).wait()
    give(0)
    pl.semaphore_wait(barrier, count)
    pipeline(
        (stage2, REDUCE[2], 0, STEPS),
        (stage1, REDUCE[1], 0, STEPS),
        (stage3, REDUCE[3], 0, STEPS),
        (stage4, REDUCE[4], 0, STEPS),
        (chain, CHAIN, 0, STEPS),
        (plane2, CHAIN + STEPS + 1, 0, 1),
        (stage0, REDUCE[0], 0, STEPS),
    )
    sums = []
    for k in range(2):
        value = last[k]
        for s in range(STEPS - 1):
            zcopy(k, s).wait_recv()
            value = value + zrecv[s, k].astype(F32)
        sums.append(value)
    for copy in flat1():
        copy.wait_recv()
    value = line[y].astype(F32)
    for i in range(3):
        value = value + liner[i].astype(F32)
    sums.append(value)
    t = time_ref[0]
    out_ref[...] = jnp.concatenate(sums, axis=0).T * (2.0 * t * (1.0 - t))

    def drain(s, carry):
        for k in range(2):
            @pl.when(s < STEPS - 1)
            def _():
                zcopy(k, s).wait_send()

            for copy in first(k, s) + near(k, s) + far(k, s) + [cross(k, s)]:
                copy.wait_send()

        @pl.when(s < STEPS - 1)
        def _():
            flatz(s).wait_send()

        flatcross(s).wait_send()
        return carry

    lax.fori_loop(0, STEPS, drain, 0)
    for copy in flat1() + flat2():
        copy.wait_send()


def reduce(key_grad, value_grad, time, hidden):
    vmem = pl.BlockSpec(memory_space=pltpu.VMEM)
    dma = pltpu.SemaphoreType.DMA
    return pl.pallas_call(
        reduce_kernel,
        name="gradient_reduce",
        out_shape=jax.ShapeDtypeStruct((128, 128), F32),
        in_specs=[vmem, vmem, pl.BlockSpec(memory_space=pltpu.SMEM), pl.BlockSpec(memory_space=pl.ANY)],
        out_specs=vmem,
        scratch_shapes=[
            pltpu.VMEM((SEQ, 4096), BF),
            pltpu.VMEM((STEPS, 2, 4, 4, PART, 128), BF),
            pltpu.VMEM((STEPS, 2, 4, 4, PART, 128), BF),
            pltpu.VMEM((4, 2, 4, 4, PART, 128), F32),
            pltpu.VMEM((STEPS, 2, 4, 4, PART, 128), BF),
            pltpu.VMEM((STEPS, 2, 4, PART, 128), BF),
            pltpu.VMEM((STEPS, 2, 2, 4, PART, 128), BF),
            pltpu.VMEM((STEPS, 2, 4, PART, 128), BF),
            pltpu.VMEM((STEPS, 2, 3, PART, 128), BF),
            pltpu.VMEM((STEPS, 2, PART, 128), BF),
            pltpu.VMEM((STEPS, 2, PART, 128), BF),
            pltpu.VMEM((2, PART, 128), F32),
            pltpu.VMEM((STEPS, 4, 4, REST, 128), BF),
            pltpu.VMEM((STEPS, 4, 4, REST, 128), BF),
            pltpu.VMEM((4, 4, 4, REST, 128), F32),
            pltpu.VMEM((STEPS, 4, 4, REST, 128), BF),
            pltpu.VMEM((STEPS, 4, 4, REST, 128), BF),
            pltpu.VMEM((3, 4, REST, 128), BF),
            pltpu.VMEM((4, REST, 128), BF),
            pltpu.VMEM((3, REST, 128), BF),
            dma((2, STEPS)), dma((2, STEPS)),
            dma((2, STEPS, 4)), dma((2, STEPS, 4)),
            dma((2, STEPS, 3)), dma((2, STEPS, 3)),
            dma((2, STEPS)), dma((2, STEPS)),
            dma((STEPS,)), dma((STEPS,)),
            dma((STEPS,)), dma((STEPS,)),
            dma((6,)), dma((6,)),
            dma((STEPS,)),
        ],
        compiler_params=pltpu.CompilerParams(collective_id=1, has_side_effects=True, vmem_limit_bytes=60 * 2**20),
    )(key_grad, value_grad, time, hidden)


def local(hidden, queries, cotangent, point_start, point_mid, point_end, curve_time):
    kv = project(point_start, point_mid, point_end, curve_time, hidden)
    context, key_grad, value_grad = attend(kv, queries, cotangent)
    return context, reduce(key_grad, value_grad, curve_time, hidden)


def solution(mesh):
    return jax.shard_map(
        local,
        mesh=mesh,
        in_specs=(
            P(("dp", "fsdp"), None),
            P(("dp", "fsdp"), None),
            P(("dp", "fsdp"), None),
            P("fsdp", "dp"),
            P("fsdp", "dp"),
            P("fsdp", "dp"),
            P(),
        ),
        out_specs=(P(("dp", "fsdp"), None), P("fsdp", "dp")),
        check_vma=False,
    )
```
